32 devices in a mesh: blk: 8 (over y, x, core), rep: 4 (over z).
Axes of the slice: x: 2, y: 2, z: 4, core: 2. Of those that a mesh axis runs over, the one named last changes fastest.
Arguments:
- anchors: float32 [3, 8192], P(None, ('blk', 'rep')), may hold values from -1 to 1
- directions: float32 [3, 8192], P(None, ('blk', 'rep')), may hold values from -4 to 4
- app_ids: int32 [8192], P(('blk', 'rep')), may hold values from 0 to 8191
- block_ids: int32 [64, 3], P(('blk', 'rep')), may hold values from 0 to 7, as said below
- color_grad: float32 [3, 8192], P(None, ('blk', 'rep')), may hold values from -6 to 6
- block_centers: float32 [3, 8], P(None, 'blk'), may hold values from -1 to 1
- pos_weight: bfloat16 [8, 256, 63], P('blk'), may hold values from -1 to 1
- trunk_weight: bfloat16 [8, 2, 256, 256], P('blk'), may hold values from -0.5 to 0.5
- density_weight: bfloat16 [8, 256], P('blk'), may hold values from -0.5 to 0.5
- feature_weight: bfloat16 [8, 128, 256], P('blk'), may hold values from -0.5 to 0.5
- view_weight: bfloat16 [8, 128, 27], P('blk'), may hold values from -1.25 to 1.25
- code_weight: bfloat16 [8, 128, 32], P('blk'), may hold values from -1 to 1
- radiance_weight: bfloat16 [8, 3, 128], P('blk'), may hold values from -0.75 to 0.75
- code_table: bfloat16 [8, 32, 8192], P('blk'), may hold values from -5 to 5
Outputs:
- colors: float32 [3, 8192], P(None, ('blk', 'rep'))
- grad_pos_weight: float32 [8, 256, 63], P('blk')
- grad_trunk_weight: float32 [8, 2, 256, 256], P('blk')
- grad_density_weight: float32 [8, 256], P('blk')
- grad_feature_weight: float32 [8, 128, 256], P('blk')
- grad_view_weight: float32 [8, 128, 27], P('blk')
- grad_code_weight: float32 [8, 128, 32], P('blk')
- grad_radiance_weight: float32 [8, 3, 128], P('blk')
- grad_code_table: float32 [8, 32, 8192], P('blk')
The draws below stay inside these ranges and needn't reach their ends.
Inputs may be any that keep to these rules, and one draw needn't show every extreme that they name: `block_ids`: each tile names three different blocks; the tiles of one device never name the same block twice; among the devices that share an index along rep, every block is named by at most 8 tiles, and some block by exactly 8 tiles.
All inputs are finite; a program needn't handle non-finite values.
Results may differ from the reference program's by a relative error of at most 0.015.
Values sent between devices are 32-bit elements; how exact they have to be, the bound alone decides.
No kernel may reach another device: no remote copies, remote signals or barrier semaphores. Data moves between devices by JAX's collectives and lax.ppermute only.
A program may use at most 64 MiB of HBM per device.

```python
import jax
import jax.numpy as jnp
from jax import lax

TILE = 128
SAMPLES = 4
HID = 256
DEPTH = 2
CHID = 128
FREQ = 10
VFREQ = 4
E = 32
APP = 8192
ENC = 63
VENC = 27
BLOCKS = 8
TILES_DEV = 2
LOAD = 8
RAYS = 8192
N_BLK = 8
N_REP = 4


def draw_block_ids(key, part):
    per_device = 3 * TILES_DEV
    block_range = jnp.arange(N_BLK, dtype=jnp.int32)

    def one_group(group_index):
        group_key = jax.random.fold_in(key, group_index + 17)
        group_keys = jax.random.split(group_key, 5)
        hottest = jax.random.randint(group_keys[0], (), 0, N_BLK)
        source_order = jax.random.permutation(group_keys[2], N_BLK)
        jitter = jax.random.randint(group_keys[3], (N_BLK, N_BLK), 0, 1 << 14)

        def choose(remaining, step_index):
            scores = (remaining > 0).astype(jnp.int32) * (1 << 28) + ((block_range == hottest) & (remaining > 0)).astype(jnp.int32) * (1 << 27) + jnp.maximum(remaining, 0) * (1 << 20) + jitter[step_index] * 64 + block_range
            _, chosen = lax.top_k(scores, per_device)
            chosen = chosen.astype(jnp.int32)
            used_now = jnp.sum((chosen[:, None] == block_range[None, :]).astype(jnp.int32), 0)
            shuffled = jax.random.permutation(jax.random.fold_in(group_keys[4], step_index), chosen)
            return (remaining - used_now, shuffled)
        _, chosen_all = lax.scan(choose, jnp.full((N_BLK,), LOAD, jnp.int32), jnp.arange(N_BLK, dtype=jnp.int32))
        return jnp.zeros((N_BLK, per_device), jnp.int32).at[source_order].set(chosen_all)
    groups = lax.map(one_group, jnp.arange(N_REP, dtype=jnp.int32))
    return groups.transpose(1, 0, 2).reshape(N_BLK * N_REP * TILES_DEV, 3)


def plant(result, key, low, top_value):
    longest = result.shape.index(max(result.shape))
    spots = []
    for shift in (0, 1):
        where = [jax.random.randint(jax.random.fold_in(key, axis), (), 0, length) for axis, length in enumerate(result.shape)]
        where[longest] = (where[longest] + shift) % result.shape[longest]
        spots.append(tuple(where))
    return result.at[spots[0]].set(low).at[spots[1]].set(top_value)


def block_levels(key, dims, cuts, least, largest):
    factor_of, own = 1.0, jax.random.fold_in(key, 6)
    for position, parts in cuts:
        draws = jnp.exp(jax.random.uniform(jax.random.fold_in(own, position), (parts,), jnp.float32, least / len(cuts), largest / len(cuts)))
        factor_of = factor_of * jnp.repeat(draws, dims[position] // parts).reshape([-1 if axis == position else 1 for axis in range(len(dims))])
    return factor_of


def gaussian(stream_key, extent, deviation, reach, shards=(), kind=jnp.bfloat16):
    loudness = block_levels(stream_key, extent, shards, -0.22, 0.18) if shards else 1.0
    values = jax.random.normal(stream_key, extent, jnp.float32) * deviation * loudness
    return jnp.minimum(jnp.maximum(values, -reach), reach).astype(kind)


def setup_inputs(seed: int = 0) -> dict:
    arg_keys = jax.random.split(jax.random.key(seed), 15)
    anchors = jnp.clip(jax.random.uniform(arg_keys[0], (3, RAYS), jnp.float32, -1.0, 1.0) * block_levels(arg_keys[0], (3, RAYS), ((1, 32),), -0.4, 0.0), -1.0, 1.0)
    directions = gaussian(arg_keys[1], (3, RAYS), 0.7, 4.0, ((1, 32),), jnp.float32)
    app_ids = plant(jax.random.randint(arg_keys[2], (RAYS,), 0, APP), jax.random.fold_in(arg_keys[2], 1), 0, APP - 1).astype(jnp.int32)
    block_ids = draw_block_ids(jax.random.fold_in(arg_keys[14], 71), 0)
    color_grad = gaussian(arg_keys[4], (3, RAYS), 1.0, 6.0, ((1, 32),), jnp.float32)
    block_centers = jnp.clip(jax.random.uniform(arg_keys[5], (3, BLOCKS), jnp.float32, -1.0, 1.0) * block_levels(arg_keys[5], (3, BLOCKS), ((1, 8),), -0.4, 0.0), -1.0, 1.0)
    pos_weight = gaussian(arg_keys[6], (BLOCKS, HID, ENC), (ENC // 2) ** -0.5, 1.0, ((0, 8),))
    trunk_weight = gaussian(arg_keys[7], (BLOCKS, DEPTH, HID, HID), (HID // 2) ** -0.5, 0.5, ((0, 8),))
    density_weight = gaussian(arg_keys[8], (BLOCKS, HID), (HID // 2) ** -0.5, 0.5, ((0, 8),))
    feature_weight = gaussian(arg_keys[9], (BLOCKS, CHID, HID), (HID // 2) ** -0.5, 0.5, ((0, 8),))
    view_weight = gaussian(arg_keys[10], (BLOCKS, CHID, VENC), VENC ** -0.5, 1.25, ((0, 8),))
    code_weight = gaussian(arg_keys[11], (BLOCKS, CHID, E), E ** -0.5, 1.0, ((0, 8),))
    radiance_weight = gaussian(arg_keys[12], (BLOCKS, 3, CHID), (CHID // 2) ** -0.5, 0.75, ((0, 8),))
    code_table = gaussian(arg_keys[13], (BLOCKS, E, APP), 1.0, 5.0, ((0, 8),))
    return {"anchors": anchors, "directions": directions, "app_ids": app_ids, "block_ids": block_ids, "color_grad": color_grad, "block_centers": block_centers, "pos_weight": pos_weight, "trunk_weight": trunk_weight, "density_weight": density_weight, "feature_weight": feature_weight, "view_weight": view_weight, "code_weight": code_weight, "radiance_weight": radiance_weight, "code_table": code_table}


ray_span = 2.0
loss_scale = 0.03125

def encode(values, levels):
    scales = 2.0 ** jnp.arange(levels).astype(values.dtype)
    angles = (scales[:, None, None] * values[None]).reshape(levels * 3, values.shape[1])
    return jnp.concatenate([values, jnp.sin(angles), jnp.cos(angles)], 0)

def render(params, code_block, center, anchor, direction, codes_row):
    pos_weight, trunk_weight, density_weight, feature_weight, view_weight, code_weight, radiance_weight = params
    ray_count = anchor.shape[1]
    spacing = ray_span / SAMPLES
    depths = (jnp.arange(SAMPLES).astype(anchor.dtype) + 0.5) * spacing
    points = anchor[:, None, :] + depths[None, :, None] * direction[:, None, :] - center[:, None, None]
    points = points.reshape(3, SAMPLES * ray_count)
    pos_code = encode(points, FREQ).astype(jnp.bfloat16)
    hidden = jax.nn.softplus(jnp.dot(pos_weight, pos_code, preferred_element_type=jnp.float32)).astype(jnp.bfloat16)
    for level_index in range(trunk_weight.shape[0]):
        hidden = jax.nn.softplus(jnp.dot(trunk_weight[level_index], hidden, preferred_element_type=jnp.float32)).astype(jnp.bfloat16)
    density = jax.nn.softplus(jnp.dot(density_weight[None, :], hidden, preferred_element_type=jnp.float32)).reshape(SAMPLES, ray_count)
    view_code = encode(direction, VFREQ).astype(jnp.bfloat16)
    app_code = jnp.take(code_block, codes_row.astype(jnp.int32), axis=1)
    per_ray = jnp.dot(view_weight, view_code, preferred_element_type=jnp.float32) + jnp.dot(code_weight, app_code, preferred_element_type=jnp.float32)
    feature = jnp.dot(feature_weight, hidden, preferred_element_type=jnp.float32).reshape(-1, SAMPLES, ray_count)
    shaded = jax.nn.softplus(feature + per_ray[:, None, :]).astype(jnp.bfloat16).reshape(-1, SAMPLES * ray_count)
    radiance = jax.nn.sigmoid(jnp.dot(radiance_weight, shaded, preferred_element_type=jnp.float32)).reshape(3, SAMPLES, ray_count)
    optical = density * spacing
    passed = jnp.exp(-(jnp.cumsum(optical, 0) - optical))
    sample_weight = passed * (1.0 - jnp.exp(-optical))
    ray_color = lax.optimization_barrier(jnp.sum(sample_weight[None] * radiance, 1))
    opacity = lax.optimization_barrier(jnp.sum(sample_weight, 0))
    offset = anchor - center[:, None]
    blend_weight = (0.1 + opacity) / (1.0 + lax.optimization_barrier(jnp.sum(offset * offset, 0)))
    return jnp.concatenate([ray_color * blend_weight[None], blend_weight[None]], 0)

def blend_colors(partials):
    return partials[:, :3] / partials[:, 3:4]

def reference(anchors, directions, app_ids, block_ids, color_grad, block_centers, pos_weight, trunk_weight, density_weight, feature_weight, view_weight, code_weight, radiance_weight, code_table):
    float_type = anchors.dtype
    tile_count = block_ids.shape[0]
    ray_tiles = jnp.concatenate([anchors, directions], 0).reshape(6, tile_count, TILE).transpose(1, 0, 2)
    code_tiles = app_ids.astype(jnp.int32).reshape(tile_count, TILE)
    block_rows = block_ids.astype(jnp.int32)
    grad_tiles = color_grad.reshape(3, tile_count, TILE).transpose(1, 0, 2)
    every_block = (pos_weight, trunk_weight, density_weight, feature_weight, view_weight, code_weight, radiance_weight)

    def block_params(block_index):
        return tuple((member[block_index] for member in every_block))

    def forward_tile(inputs):
        ray_rows, codes_row, blocks_row = inputs
        running = jnp.zeros((4, TILE), float_type)
        for slot_index in range(3):
            block_index = blocks_row[slot_index].astype(jnp.int32)
            piece = render(block_params(block_index), code_table[block_index], block_centers[:, block_index], ray_rows[:3], ray_rows[3:], codes_row)
            running = running + piece.astype(float_type)
        return running
    partials = lax.map(forward_tile, (ray_tiles, code_tiles, block_rows))
    ray_colors, pullback = jax.vjp(blend_colors, partials)
    cot_parts, = pullback((grad_tiles * loss_scale).astype(partials.dtype))

    def backward_tile(totals, inputs):
        ray_rows, codes_row, blocks_row, cot_row = inputs
        for slot_index in range(3):
            block_index = blocks_row[slot_index].astype(jnp.int32)
            center = block_centers[:, block_index]

            def local_render(weights, code_block):
                return render(weights, code_block, center, ray_rows[:3], ray_rows[3:], codes_row)
            _, pull_back = jax.vjp(local_render, block_params(block_index), code_table[block_index])
            grad_params, grad_block = pull_back(cot_row)
            pieces = tuple(grad_params) + (grad_block,)
            totals = tuple((running.at[block_index].add(piece_grad.astype(running.dtype)) for running, piece_grad in zip(totals, pieces)))
        return (totals, None)
    start = tuple((jnp.zeros(member.shape, float_type) for member in every_block + (code_table,)))
    totals, _ = lax.scan(backward_tile, start, (ray_tiles, code_tiles, block_rows, cot_parts))
    colors = ray_colors.transpose(1, 0, 2).reshape(3, tile_count * TILE)
    return (colors, totals[0], totals[1], totals[2], totals[3], totals[4], totals[5], totals[6], totals[7])
```

```python
import functools

import jax
import jax.numpy as jnp
from jax import lax
from jax.experimental import pallas as pl
from jax.experimental.pallas import tpu as pltpu
from jax.sharding import PartitionSpec as P

TILE = 128
SAMPLES = 4
FREQ = 10
VFREQ = 4
COLS = SAMPLES * TILE
LOW = 256
ROWS = 16
VCODE = 32
EDGE = 144
DENSE = 131

ray_span = 2.0
loss_scale = 0.03125
spacing = ray_span / SAMPLES

F32 = jnp.float32
BF16 = jnp.bfloat16


def dot(a, b):
    return lax.dot_general(a, b, (((1,), (0,)), ((), ())), preferred_element_type=F32)


def dot_nt(a, b):
    return lax.dot_general(a, b, (((1,), (1,)), ((), ())), preferred_element_type=F32)


def vmem():
    return pl.BlockSpec(memory_space=pltpu.VMEM)


def smem():
    return pl.BlockSpec(memory_space=pltpu.SMEM)


def whole(shape):
    return pl.BlockSpec(shape, lambda i: (0,) * len(shape))


def sin_cos(angle, is_cos):
    turns = jnp.floor(angle * 0.6366197723675814 + 0.5)
    rest = angle - turns * 1.5703125
    rest = rest - turns * 4.837512969970703125e-4
    rest = rest - turns * 7.54978995489188216e-8
    quarter = turns.astype(jnp.int32) + is_cos
    sq = rest * rest
    sine = rest + rest * sq * (
        -1.6666654611e-1 + sq * (8.3321608736e-3 + sq * -1.9515295891e-4)
    )
    cosine = (
        1.0
        - 0.5 * sq
        + sq * sq * (4.166664568298827e-2 + sq * (-1.388731625493765e-3 + sq * 2.443315711809948e-5))
    )
    value = jnp.where((quarter & 1) == 1, cosine, sine)
    return jnp.where((quarter & 2) == 2, -value, value)


def encode(coords, levels, rows):
    n = coords[0].shape[1]
    row = lax.broadcasted_iota(jnp.int32, (rows, n), 0)
    third = (row * 171) >> 9
    coord = row - 3 * third
    base = jnp.where(coord == 0, coords[0], jnp.where(coord == 1, coords[1], coords[2]))
    is_cos = (third > levels).astype(jnp.int32)
    level = jnp.clip(third - 1 - levels * is_cos, 0, levels - 1)
    scale = (1 << level).astype(F32)
    return jnp.where(third == 0, base, sin_cos(base * scale, is_cos))


def softplus(v):
    return jnp.maximum(v, 0.0) + jnp.log(1.0 + jnp.exp(-jnp.abs(v)))


def slope(h):
    return 1.0 - jnp.exp(-h.astype(F32))


def send_kernel(tiles, ids_ref, anchor_ref, dir_ref, app_ref, grad_ref, out_ref, tile_ref):
    row = lax.broadcasted_iota(jnp.int32, out_ref.shape, 1)
    out_ref[...] = jnp.where((row >= 10) & (row < 13), -1.0, 0.0)
    for t in range(tiles):
        lanes = pl.ds(t * TILE, TILE)
        tile_ref[t] = jnp.zeros((ROWS, TILE), F32)
        tile_ref[t, 0:3, :] = anchor_ref[:, lanes]
        tile_ref[t, 3:6, :] = dir_ref[:, lanes]
        tile_ref[t, 6:7, :] = app_ref[t : t + 1, :].astype(F32)
        tile_ref[t, 7:10, :] = grad_ref[:, lanes]
        for k in range(3):
            tile_ref[t, 10 + k : 11 + k, :] = jnp.full((1, TILE), ids_ref[t, k], jnp.int32).astype(F32)
        for k in range(3):
            out_ref[ids_ref[t, k]] = tile_ref[t]


def weight_kernel(tw_ref, wfd_ref, wvc_ref, wr_ref, table_ref, w0t, w1t, wfdt, wct, wrt, stack):
    w0t[...] = tw_ref[0].T
    w1t[...] = tw_ref[1].T
    wfdt[...] = wfd_ref[...].T
    wct[...] = wvc_ref[...].T[0 : wct.shape[0]]
    wrt[...] = wr_ref[...].T
    codes = table_ref.shape[0]
    for hi in range(table_ref.shape[1] // LOW):
        stack[hi * codes : (hi + 1) * codes, :] = table_ref[:, hi * LOW : (hi + 1) * LOW]


def composite(density, radiance):
    decay = [jnp.exp(-d * spacing) for d in density]
    passed, run = [], jnp.zeros_like(density[0])
    for d in density:
        passed.append(jnp.exp(-run))
        run = run + d * spacing
    weight = [p * (1.0 - e) for p, e in zip(passed, decay)]
    color = [sum(w * r for w, r in zip(weight, radiance[c])) for c in range(3)]
    return decay, passed, weight, color, sum(weight)


def distance(rays, centers):
    total = 1.0
    for c in range(3):
        offset = rays[:, c, :] - centers[c, 0]
        total = total + offset * offset
    return total


def forward_kernel(
    group, codes, rays_ref, center_ref, wp, tw, wfd, wvc, wr, stack,
    partial_ref, code_ref, h0_ref, h1_ref, h2_ref, shade_ref, vc_ref, density_ref, radiance_ref,
    dl_scr, rl_scr,
):
    step = pl.program_id(0)
    highs = stack.shape[0] // codes
    for j in range(group):
        tile = step * group + j
        at = slice(j * COLS, (j + 1) * COLS)
        rays = rays_ref[tile]
        points = []
        for c in range(3):
            base = rays[c : c + 1, :]
            move = rays[3 + c : 4 + c, :]
            points.append(
                jnp.concatenate(
                    [base + ((s + 0.5) * spacing) * move - center_ref[c, 0] for s in range(SAMPLES)], 1
                )
            )
        code = encode(points, FREQ, wp.shape[1]).astype(BF16)
        code_ref[:, at] = code
        h0 = softplus(dot(wp[...], code)).astype(BF16)
        h0_ref[:, at] = h0
        h1 = softplus(dot(tw[0], h0)).astype(BF16)
        h1_ref[:, at] = h1
        h2 = softplus(dot(tw[1], h1)).astype(BF16)
        h2_ref[:, at] = h2
        feature = dot(wfd[...], h2)
        dl_scr[pl.ds(tile, 1), :] = feature[DENSE : DENSE + 1, :]
        view = encode([rays[3 + c : 4 + c, :] for c in range(3)], VFREQ, VCODE)
        ids = rays[6:7, :].astype(jnp.int32)
        low, high = ids & (LOW - 1), ids // LOW
        hit = (lax.broadcasted_iota(jnp.int32, (LOW, TILE), 0) == low).astype(F32).astype(BF16)
        picked = dot(stack[...], hit)
        app = jnp.zeros((codes, TILE), F32)
        for hi in range(highs):
            app = app + jnp.where(high == hi, picked[hi * codes : (hi + 1) * codes], 0.0)
        vc = jnp.concatenate([app, view], 0).astype(BF16)
        vc_ref[:, j * TILE : (j + 1) * TILE] = vc
        per_ray = dot(wvc[...], vc)
        shaded = softplus(feature[0:128] + jnp.concatenate([per_ray] * SAMPLES, 1)).astype(BF16)
        shade_ref[:, at] = shaded
        logits = dot(wr[...], shaded)
        for c in range(3):
            rl_scr[c, pl.ds(tile, 1), :] = logits[c : c + 1, :]

    @pl.when(step == pl.num_programs(0) - 1)
    def _():
        logit = dl_scr[...]
        density = jnp.maximum(logit, 0.0) + jnp.log1p(jnp.exp(-jnp.abs(logit)))
        density_ref[0] = density
        density_ref[1] = 1.0 / (1.0 + jnp.exp(-logit))
        radiance = [1.0 / (1.0 + jnp.exp(-rl_scr[c])) for c in range(3)]
        for c in range(3):
            radiance_ref[c] = radiance[c]
        lanes = [slice(s * TILE, (s + 1) * TILE) for s in range(SAMPLES)]
        _, _, _, color, opacity = composite(
            [density[:, at] for at in lanes], [[radiance[c][:, at] for at in lanes] for c in range(3)]
        )
        share = (0.1 + opacity) / distance(rays_ref, center_ref)
        for c in range(3):
            partial_ref[c] = share * color[c]
        partial_ref[3] = share


def cotangents(rays_ref, center_ref, parts_ref, density_ref, radiance_ref, cot_scr):
    ids = [rays_ref[:, 10 + k, :] for k in range(3)]
    live = ids[0] >= 0.0
    summed = [jnp.zeros_like(ids[0]) for _ in range(4)]
    for b in range(parts_ref.shape[0]):
        mine = (ids[0] == b) | (ids[1] == b) | (ids[2] == b)
        for c in range(4):
            summed[c] = summed[c] + jnp.where(mine, parts_ref[b, c], 0.0)
    norm = 1.0 / jnp.where(live, summed[3], 1.0)
    got = [jnp.where(live, rays_ref[:, 7 + c, :] * loss_scale, 0.0) * norm for c in range(3)]
    got_share = -sum(got[c] * summed[c] for c in range(3)) * norm
    lanes = [slice(s * TILE, (s + 1) * TILE) for s in range(SAMPLES)]
    density = [density_ref[0, :, at] for at in lanes]
    gate = [density_ref[1, :, at] for at in lanes]
    radiance = [[radiance_ref[c, :, at] for at in lanes] for c in range(3)]
    decay, passed, weight, color, opacity = composite(density, radiance)
    far = 1.0 / distance(rays_ref, center_ref)
    share = (0.1 + opacity) * far
    d_color = [got[c] * share for c in range(3)]
    d_opacity = (sum(got[c] * color[c] for c in range(3)) + got_share) * far
    d_weight = [
        sum(d_color[c] * radiance[c][s] for c in range(3)) + d_opacity for s in range(SAMPLES)
    ]
    later = jnp.zeros_like(far)
    cot_scr[...] = jnp.zeros_like(cot_scr)
    for s in reversed(range(SAMPLES)):
        d_optical = passed[s] * decay[s] * d_weight[s] - later
        later = later + weight[s] * d_weight[s]
        cot_scr[:, 3, lanes[s]] = d_optical * spacing * gate[s]
        for c in range(3):
            r = radiance[c][s]
            cot_scr[:, c, lanes[s]] = d_color[c] * weight[s] * r * (1.0 - r)


def backward_kernel(
    group, tiles, ids_ref, me_ref, rays_ref, center_ref, parts_ref, density_ref, radiance_ref,
    code_ref, h0_ref, h1_ref, h2_ref, shade_ref, vc_ref, w0t, w1t, wfdt, wct, wrt,
    colors_ref, head_ref, g1_ref, g0_ref, gp_ref, column_ref,
    cot_scr, fd_scr, r_scr, vc_scr,
):
    step = pl.program_id(0)

    @pl.when(step == 0)
    def _():
        cotangents(rays_ref, center_ref, parts_ref, density_ref, radiance_ref, cot_scr)
        me = me_ref[0]
        for t in range(tiles):
            summed = [
                sum(parts_ref[ids_ref[t, k], c, pl.ds(me, 1), :] for k in range(3)) for c in range(4)
            ]
            for c in range(3):
                colors_ref[c : c + 1, t * TILE : (t + 1) * TILE] = summed[c] / summed[3]
        for ref in (g1_ref, g0_ref, gp_ref, fd_scr, r_scr, vc_scr):
            ref[...] = jnp.zeros_like(ref)

    for j in range(group):
        tile = step * group + j
        at = slice(j * COLS, (j + 1) * COLS)
        cot = cot_scr[tile]
        low = jnp.concatenate([cot, jnp.zeros_like(cot)], 0).astype(BF16)
        shaded = shade_ref[:, at]
        d_feature = dot(wrt[...], low) * slope(shaded)
        r_scr[...] += dot_nt(low, shaded)
        d_ray = (
            d_feature[:, 0:TILE]
            + d_feature[:, TILE : 2 * TILE]
            + d_feature[:, 2 * TILE : 3 * TILE]
            + d_feature[:, 3 * TILE :]
        ).astype(BF16)
        vc = vc_ref[:, j * TILE : (j + 1) * TILE]
        vc_scr[...] += dot_nt(vc, d_ray)
        column_ref[:, j * TILE : (j + 1) * TILE] = dot(wct[...], d_ray).astype(BF16).astype(F32)
        h2 = h2_ref[:, at]
        edge = jnp.concatenate([d_feature.astype(BF16), low], 0)
        fd_scr[...] += dot_nt(edge, h2)
        d2 = (dot(wfdt[...], edge) * slope(h2)).astype(BF16)
        h1 = h1_ref[:, at]
        g1_ref[...] += dot_nt(d2, h1)
        d1 = (dot(w1t[...], d2) * slope(h1)).astype(BF16)
        h0 = h0_ref[:, at]
        g0_ref[...] += dot_nt(d1, h0)
        d0 = (dot(w0t[...], d1) * slope(h0)).astype(BF16)
        gp_ref[...] += dot_nt(code_ref[:, at], d0)

    @pl.when(step == pl.num_programs(0) - 1)
    def _():
        head_ref[0:EDGE, :] = fd_scr[...]
        head_ref[EDGE - 8 : EDGE, 0:128] = r_scr[0:8, :]
        half = vc_scr.shape[0] // 2
        head_ref[EDGE : EDGE + half, 0:128] = vc_scr[0:half, :]
        head_ref[EDGE : EDGE + half, 128:256] = vc_scr[half:, :]


def table_kernel(
    side_ref, own_ref, near_ref, far0_ref, far1_ref, ids_ref, out_ref, cols, lhs, total
):
    side = side_ref[0]
    codes, rays = own_ref.shape
    upper = (side >= 2).astype(jnp.int32)
    cols[side] = own_ref[...]
    cols[side + 1 - 2 * (side & 1)] = near_ref[...]
    cols[2 - upper] = far0_ref[...]
    cols[3 - 3 * upper] = far1_ref[...]
    highs = out_ref.shape[1] // LOW
    chunk = lhs.shape[1]
    total[...] = jnp.zeros_like(total)
    for z in range(4):
        for start in range(0, rays, chunk):
            ids = ids_ref[z, :, start : start + chunk]
            low, high = ids & (LOW - 1), ids // LOW
            value = cols[z, :, start : start + chunk].astype(BF16)
            for hi in range(highs):
                lhs[hi * codes : (hi + 1) * codes, :] = jnp.where(high == hi, value, jnp.zeros_like(value))
            hit = (lax.broadcasted_iota(jnp.int32, (LOW, chunk), 0) == low).astype(F32).astype(BF16)
            total[...] += dot_nt(lhs[...], hit)
    for hi in range(highs):
        out_ref[:, hi * LOW : (hi + 1) * LOW] = total[hi * codes : (hi + 1) * codes]


def finish_kernel(
    views, side_ref, a0, a1, b0, b1, c0, c1, d0, d1,
    pos_ref, trunk_ref, density_ref, feature_ref, view_ref, code_ref, rad_ref,
):
    inner = (side_ref[0] == 1) | (side_ref[0] == 2)

    def pick(total, sent):
        return jnp.where(inner, total[...], sent[...])

    trunk_ref[1] = pick(b0, b1)
    trunk_ref[0] = pick(c0, c1)
    pos_ref[...] = pick(d0, d1).T[:, 0 : pos_ref.shape[1]]
    head = pick(a0, a1)
    feature_ref[...] = head[0:128]
    density_ref[...] = head[DENSE : DENSE + 1]
    rad_ref[...] = head[EDGE - 8 : EDGE - 5, 0:128]
    code_ref[...] = head[EDGE : EDGE + VCODE, 0:128].T
    view_ref[...] = head[EDGE : EDGE + VCODE, 128:256].T[:, 0:views]


def shape_of(*dims, dtype=F32):
    return jax.ShapeDtypeStruct(dims, dtype)


def local(
    anchors,
    directions,
    app_ids,
    block_ids,
    color_grad,
    block_centers,
    pos_weight,
    trunk_weight,
    density_weight,
    feature_weight,
    view_weight,
    code_weight,
    radiance_weight,
    code_table,
):
    tiles = block_ids.shape[0]
    blocks = lax.axis_size("blk")
    reps = lax.axis_size("rep")
    assert reps == 4
    group = 2 if blocks % 2 == 0 else 1
    hid = pos_weight.shape[1]
    codes, entries = code_table.shape[1:]
    params = pltpu.CompilerParams(vmem_limit_bytes=60000 * 1024)

    send = pl.pallas_call(
        functools.partial(send_kernel, tiles),
        out_shape=shape_of(blocks, ROWS, TILE),
        in_specs=[smem()] + [vmem()] * 4,
        out_specs=vmem(),
        scratch_shapes=[pltpu.VMEM((tiles, ROWS, TILE), F32)],
        name="send",
    )(block_ids, anchors, directions, app_ids.reshape(tiles, TILE), color_grad)
    rays = lax.all_to_all(send, "blk", split_axis=0, concat_axis=0, tiled=True)

    wp = jnp.pad(pos_weight[0], ((0, 0), (0, 64 - pos_weight.shape[2])))
    trunk = trunk_weight[0]
    wfd = jnp.concatenate(
        [
            feature_weight[0],
            jnp.zeros((DENSE - 128, hid), BF16),
            density_weight,
            jnp.zeros((EDGE - DENSE - 1, hid), BF16),
        ],
        0,
    )
    wvc = jnp.concatenate(
        [code_weight[0], view_weight[0], jnp.zeros((128, VCODE - view_weight.shape[2]), BF16)], 1
    )
    wr = jnp.pad(radiance_weight[0], ((0, 13), (0, 0)))
    w0t, w1t, wfdt, wct, wrt, stack = pl.pallas_call(
        weight_kernel,
        out_shape=(
            shape_of(hid, hid, dtype=BF16),
            shape_of(hid, hid, dtype=BF16),
            shape_of(hid, EDGE, dtype=BF16),
            shape_of(codes, 128, dtype=BF16),
            shape_of(128, 16, dtype=BF16),
            shape_of(entries // LOW * codes, LOW, dtype=BF16),
        ),
        in_specs=[vmem()] * 5,
        out_specs=(vmem(),) * 6,
        name="weights",
    )(trunk, wfd, wvc, wr, code_table[0])

    n = blocks * COLS
    steps = blocks // group
    wide = lambda rows, cols: pl.BlockSpec((rows, group * cols), lambda i: (0, i))
    saved_shapes = (
        shape_of(64, n, dtype=BF16),
        shape_of(hid, n, dtype=BF16),
        shape_of(hid, n, dtype=BF16),
        shape_of(hid, n, dtype=BF16),
        shape_of(128, n, dtype=BF16),
        shape_of(64, blocks * TILE, dtype=BF16),
        shape_of(2, blocks, COLS),
        shape_of(3, blocks, COLS),
    )
    saved_specs = (
        wide(64, COLS),
        wide(hid, COLS),
        wide(hid, COLS),
        wide(hid, COLS),
        wide(128, COLS),
        wide(64, TILE),
        whole((2, blocks, COLS)),
        whole((3, blocks, COLS)),
    )
    outs = pl.pallas_call(
        functools.partial(forward_kernel, group, codes),
        grid=(steps,),
        out_shape=(shape_of(4, blocks, TILE),) + saved_shapes,
        in_specs=[
            whole(rays.shape),
            smem(),
            whole(wp.shape),
            whole(trunk.shape),
            whole(wfd.shape),
            whole(wvc.shape),
            whole(wr.shape),
            whole(stack.shape),
        ],
        out_specs=(whole((4, blocks, TILE)),) + saved_specs,
        scratch_shapes=[pltpu.VMEM((blocks, COLS), F32), pltpu.VMEM((3, blocks, COLS), F32)],
        compiler_params=params,
        name="forward",
    )(rays, block_centers, wp, trunk, wfd, wvc, wr, stack)
    partial, saved = outs[0], outs[1:]
    code, h0, h1, h2, shaded, vc, density, radiance = saved
    parts = lax.all_gather(partial, "blk", axis=0, tiled=False)

    me = lax.axis_index("blk").astype(jnp.int32)[None]
    side = lax.axis_index("rep").astype(jnp.int32)[None]
    weights_t = (w0t, w1t, wfdt, wct, wrt)
    head_rows = EDGE + VCODE
    colors, head, g1, g0, gp, columns = pl.pallas_call(
        functools.partial(backward_kernel, group, tiles),
        grid=(steps,),
        out_shape=(
            shape_of(3, tiles * TILE),
            shape_of(head_rows, hid),
            shape_of(hid, hid),
            shape_of(hid, hid),
            shape_of(64, hid),
            shape_of(codes, blocks * TILE),
        ),
        in_specs=[smem(), smem(), whole(rays.shape), smem(), whole(parts.shape)]
        + [saved_specs[6], saved_specs[7]]
        + list(saved_specs[:6])
        + [whole(w.shape) for w in weights_t],
        out_specs=(
            whole((3, tiles * TILE)),
            whole((head_rows, hid)),
            whole((hid, hid)),
            whole((hid, hid)),
            whole((64, hid)),
            wide(codes, TILE),
        ),
        scratch_shapes=[
            pltpu.VMEM((blocks, 8, COLS), F32),
            pltpu.VMEM((EDGE, hid), F32),
            pltpu.VMEM((16, 128), F32),
            pltpu.VMEM((64, 128), F32),
        ],
        compiler_params=params,
        name="backward",
    )(
        block_ids, me, rays, block_centers, parts, density, radiance,
        code, h0, h1, h2, shaded, vc, *weights_t,
    )

    swap = lambda x: lax.ppermute(x, "rep", [(0, 1), (1, 0), (2, 3), (3, 2)])
    inward = lambda x: lax.ppermute(x, "rep", [(0, 1), (3, 2)])
    middle = lambda x: lax.ppermute(x, "rep", [(1, 2), (2, 1)])
    outward = lambda x: lax.ppermute(x, "rep", [(1, 0), (2, 3)])
    is_inner = (side[0] == 1) | (side[0] == 2)

    my_ids = rays[:, 6, :].astype(jnp.int32).reshape(1, 1, blocks * TILE)
    every_ids = jnp.zeros((reps, 1, blocks * TILE), jnp.int32)
    every_ids = lax.dynamic_update_slice(every_ids, my_ids, (side[0], 0, 0))
    for shift in range(1, reps):
        moved = lax.ppermute(my_ids, "rep", [(z, (z + shift) % reps) for z in range(reps)])
        every_ids = lax.dynamic_update_slice(every_ids, moved, ((side[0] - shift) % reps, 0, 0))

    near = swap(columns)
    far = []
    for piece in (columns, near):
        got = middle(piece)
        sent = outward(got)
        far.append(jnp.where(is_inner, got, sent))

    def line_sum(grad):
        pair = grad + inward(grad)
        total = pair + middle(pair)
        return total, outward(total)

    sums = [line_sum(g) for g in (head, g1, g0, gp)]
    rays_n = blocks * TILE
    chunk = min(rays_n, 1024)
    table_grad = pl.pallas_call(
        table_kernel,
        out_shape=shape_of(codes, entries),
        in_specs=[smem()] + [vmem()] * 5,
        out_specs=vmem(),
        scratch_shapes=[
            pltpu.VMEM((reps, codes, rays_n), F32),
            pltpu.VMEM((entries // LOW * codes, chunk), BF16),
            pltpu.VMEM((entries // LOW * codes, LOW), F32),
        ],
        compiler_params=params,
        name="table",
    )(side, columns, near, far[0], far[1], every_ids)

    views = view_weight.shape[2]
    outs = pl.pallas_call(
        functools.partial(finish_kernel, views),
        out_shape=(
            shape_of(hid, pos_weight.shape[2]),
            shape_of(2, hid, hid),
            shape_of(1, hid),
            shape_of(128, hid),
            shape_of(128, views),
            shape_of(128, codes),
            shape_of(3, 128),
        ),
        in_specs=[smem()] + [vmem()] * 8,
        out_specs=(vmem(),) * 7,
        compiler_params=params,
        name="finish",
    )(side, *[x for pair in sums for x in pair])
    return (
        colors,
        outs[0][None],
        outs[1][None],
        outs[2],
        outs[3][None],
        outs[4][None],
        outs[5][None],
        outs[6][None],
        table_grad[None],
    )


def solution(mesh):
    return jax.shard_map(
        local,
        mesh=mesh,
        in_specs=(
            P(None, ("blk", "rep")),
            P(None, ("blk", "rep")),
            P(("blk", "rep")),
            P(("blk", "rep"), None),
            P(None, ("blk", "rep")),
            P(None, "blk"),
            P("blk", None, None),
            P("blk", None, None, None),
            P("blk", None),
            P("blk", None, None),
            P("blk", None, None),
            P("blk", None, None),
            P("blk", None, None),
            P("blk", None, None),
        ),
        out_specs=(
            P(None, ("blk", "rep")),
            P("blk", None, None),
            P("blk", None, None, None),
            P("blk", None),
            P("blk", None, None),
            P("blk", None, None),
            P("blk", None, None),
            P("blk", None, None),
            P("blk", None, None),
        ),
        check_vma=False,
    )
```

```python
import functools

import jax
import jax.numpy as jnp
from jax import lax
from jax.experimental import pallas as pl
from jax.experimental.pallas import tpu as pltpu
from jax.sharding import PartitionSpec as P


TILE = 128
SAMPLES = 4
FREQ = 10
VFREQ = 4
COLS = SAMPLES * TILE
LOW = 256
ROWS = 16
VCODE = 32
EDGE = 144
DENSE = 131

ray_span = 2.0
loss_scale = 0.03125
spacing = ray_span / SAMPLES

F32 = jnp.float32
BF16 = jnp.bfloat16


def dot(a, b):
    return lax.dot_general(a, b, (((1,), (0,)), ((), ())), preferred_element_type=F32)


def dot_nt(a, b):
    return lax.dot_general(a, b, (((1,), (1,)), ((), ())), preferred_element_type=F32)


def vmem():
    return pl.BlockSpec(memory_space=pltpu.VMEM)


def smem():
    return pl.BlockSpec(memory_space=pltpu.SMEM)


def whole(shape):
    return pl.BlockSpec(shape, lambda i: (0,) * len(shape))


def sin_cos(angle, is_cos):
    turns = jnp.floor(angle * 0.6366197723675814 + 0.5)
    rest = angle - turns * 1.5703125
    rest = rest - turns * 4.837512969970703125e-4
    rest = rest - turns * 7.54978995489188216e-8
    quarter = turns.astype(jnp.int32) + is_cos
    sq = rest * rest
    sine = rest + rest * sq * (
        -1.6666654611e-1 + sq * (8.3321608736e-3 + sq * -1.9515295891e-4)
    )
    cosine = (
        1.0
        - 0.5 * sq
        + sq * sq * (4.166664568298827e-2 + sq * (-1.388731625493765e-3 + sq * 2.443315711809948e-5))
    )
    value = jnp.where((quarter & 1) == 1, cosine, sine)
    return jnp.where((quarter & 2) == 2, -value, value)


def encode(coords, levels, rows):
    n = coords[0].shape[1]
    row = lax.broadcasted_iota(jnp.int32, (rows, n), 0)
    third = (row * 171) >> 9
    coord = row - 3 * third
    base = jnp.where(coord == 0, coords[0], jnp.where(coord == 1, coords[1], coords[2]))
    is_cos = (third > levels).astype(jnp.int32)
    level = jnp.clip(third - 1 - levels * is_cos, 0, levels - 1)
    scale = (1 << level).astype(F32)
    return jnp.where(third == 0, base, sin_cos(base * scale, is_cos))


def softplus(v):
    return jnp.maximum(v, 0.0) + jnp.log(1.0 + jnp.exp(-jnp.abs(v)))


def slope(h):
    return 1.0 - jnp.exp(-h.astype(F32))


def send_kernel(tiles, ids_ref, anchor_ref, dir_ref, app_ref, grad_ref, out_ref, tile_ref):
    row = lax.broadcasted_iota(jnp.int32, out_ref.shape, 1)
    out_ref[...] = jnp.where((row >= 10) & (row < 13), -1.0, 0.0)
    for t in range(tiles):
        lanes = pl.ds(t * TILE, TILE)
        tile_ref[t] = jnp.zeros((ROWS, TILE), F32)
        tile_ref[t, 0:3, :] = anchor_ref[:, lanes]
        tile_ref[t, 3:6, :] = dir_ref[:, lanes]
        tile_ref[t, 6:7, :] = app_ref[t : t + 1, :].astype(F32)
        tile_ref[t, 7:10, :] = grad_ref[:, lanes]
        for k in range(3):
            tile_ref[t, 10 + k : 11 + k, :] = jnp.full((1, TILE), ids_ref[t, k], jnp.int32).astype(F32)
        for k in range(3):
            out_ref[ids_ref[t, k]] = tile_ref[t]


def weight_kernel(
    pos_ref, tw_ref, density_ref, feature_ref, view_ref, cw_ref, rad_ref, table_ref,
    wp, wfd, wvc, wr, stack, w0t, w1t, wfdt, wct, wrt, pad, narrow,
):
    pad[...] = jnp.zeros_like(pad)
    pad[0 : pos_ref.shape[0], :] = pos_ref[...].astype(F32)
    wp[...] = pad[...].T.astype(BF16)
    narrow[...] = jnp.zeros_like(narrow)
    narrow[0 : cw_ref.shape[0], :] = cw_ref[...].astype(F32)
    narrow[cw_ref.shape[0] : cw_ref.shape[0] + view_ref.shape[0], :] = view_ref[...].astype(F32)
    wvc[...] = narrow[...].T.astype(BF16)
    wct[...] = cw_ref[...]
    wfd[0:128, :] = feature_ref[...]
    pad[0:16, :] = jnp.zeros((16, pad.shape[1]), F32)
    pad[DENSE - 128 : DENSE - 127, :] = density_ref[...].astype(F32)
    wfd[128:EDGE, :] = pad[0 : EDGE - 128, :].astype(BF16)
    narrow[0:16, :] = jnp.zeros((16, narrow.shape[1]), F32)
    narrow[0 : rad_ref.shape[0], :] = rad_ref[...].astype(F32)
    wr[...] = narrow[0:16, :].astype(BF16)
    wrt[...] = wr[...].T
    wfdt[...] = wfd[...].T
    w0t[...] = tw_ref[0].T
    w1t[...] = tw_ref[1].T
    codes = table_ref.shape[0]
    for hi in range(table_ref.shape[1] // LOW):
        stack[hi * codes : (hi + 1) * codes, :] = table_ref[:, hi * LOW : (hi + 1) * LOW]


def composite(density, radiance):
    decay = [jnp.exp(-d * spacing) for d in density]
    passed, run = [], jnp.zeros_like(density[0])
    for d in density:
        passed.append(jnp.exp(-run))
        run = run + d * spacing
    weight = [p * (1.0 - e) for p, e in zip(passed, decay)]
    color = [sum(w * r for w, r in zip(weight, radiance[c])) for c in range(3)]
    return decay, passed, weight, color, sum(weight)


def distance(rays, centers):
    total = 1.0
    for c in range(3):
        offset = rays[:, c, :] - centers[0, c]
        total = total + offset * offset
    return total


def forward_kernel(
    group, codes, rays_ref, center_ref, wp, tw, wfd, wvc, wr, stack,
    partial_ref, code_ref, h0_ref, h1_ref, h2_ref, shade_ref, vc_ref, density_ref, radiance_ref,
    dl_scr, rl_scr,
):
    step = pl.program_id(0)
    highs = stack.shape[0] // codes
    for j in range(group):
        tile = step * group + j
        at = slice(j * COLS, (j + 1) * COLS)
        rays = rays_ref[tile]
        points = []
        for c in range(3):
            base = rays[c : c + 1, :]
            move = rays[3 + c : 4 + c, :]
            points.append(
                jnp.concatenate(
                    [base + ((s + 0.5) * spacing) * move - center_ref[0, c] for s in range(SAMPLES)], 1
                )
            )
        code = encode(points, FREQ, wp.shape[1]).astype(BF16)
        code_ref[:, at] = code
        h0 = softplus(dot(wp[...], code)).astype(BF16)
        h0_ref[:, at] = h0
        h1 = softplus(dot(tw[0], h0)).astype(BF16)
        h1_ref[:, at] = h1
        h2 = softplus(dot(tw[1], h1)).astype(BF16)
        h2_ref[:, at] = h2
        feature = dot(wfd[...], h2)
        dl_scr[pl.ds(tile, 1), :] = feature[DENSE : DENSE + 1, :]
        view = encode([rays[3 + c : 4 + c, :] for c in range(3)], VFREQ, VCODE)
        ids = rays[6:7, :].astype(jnp.int32)
        low, high = ids & (LOW - 1), ids // LOW
        hit = (lax.broadcasted_iota(jnp.int32, (LOW, TILE), 0) == low).astype(F32).astype(BF16)
        picked = dot(stack[...], hit)
        app = jnp.zeros((codes, TILE), F32)
        for hi in range(highs):
            app = app + jnp.where(high == hi, picked[hi * codes : (hi + 1) * codes], 0.0)
        vc = jnp.concatenate([app, view], 0).astype(BF16)
        vc_ref[:, j * TILE : (j + 1) * TILE] = vc
        per_ray = dot(wvc[...], vc)
        shaded = softplus(feature[0:128] + jnp.concatenate([per_ray] * SAMPLES, 1)).astype(BF16)
        shade_ref[:, at] = shaded
        logits = dot(wr[...], shaded)
        for c in range(3):
            rl_scr[c, pl.ds(tile, 1), :] = logits[c : c + 1, :]

    @pl.when(step == pl.num_programs(0) - 1)
    def _():
        logit = dl_scr[...]
        density = jnp.maximum(logit, 0.0) + jnp.log1p(jnp.exp(-jnp.abs(logit)))
        density_ref[0] = density
        density_ref[1] = 1.0 / (1.0 + jnp.exp(-logit))
        radiance = [1.0 / (1.0 + jnp.exp(-rl_scr[c])) for c in range(3)]
        for c in range(3):
            radiance_ref[c] = radiance[c]
        lanes = [slice(s * TILE, (s + 1) * TILE) for s in range(SAMPLES)]
        _, _, _, color, opacity = composite(
            [density[:, at] for at in lanes], [[radiance[c][:, at] for at in lanes] for c in range(3)]
        )
        share = (0.1 + opacity) / distance(rays_ref, center_ref)
        for c in range(3):
            partial_ref[c] = share * color[c]
        partial_ref[3] = share


def cotangents(rays_ref, center_ref, parts_ref, density_ref, radiance_ref, cot_scr):
    ids = [rays_ref[:, 10 + k, :] for k in range(3)]
    live = ids[0] >= 0.0
    summed = [jnp.zeros_like(ids[0]) for _ in range(4)]
    for b in range(parts_ref.shape[0]):
        mine = (ids[0] == b) | (ids[1] == b) | (ids[2] == b)
        for c in range(4):
            summed[c] = summed[c] + jnp.where(mine, parts_ref[b, c], 0.0)
    norm = 1.0 / jnp.where(live, summed[3], 1.0)
    got = [jnp.where(live, rays_ref[:, 7 + c, :] * loss_scale, 0.0) * norm for c in range(3)]
    got_share = -sum(got[c] * summed[c] for c in range(3)) * norm
    lanes = [slice(s * TILE, (s + 1) * TILE) for s in range(SAMPLES)]
    density = [density_ref[0, :, at] for at in lanes]
    gate = [density_ref[1, :, at] for at in lanes]
    radiance = [[radiance_ref[c, :, at] for at in lanes] for c in range(3)]
    decay, passed, weight, color, opacity = composite(density, radiance)
    far = 1.0 / distance(rays_ref, center_ref)
    share = (0.1 + opacity) * far
    d_color = [got[c] * share for c in range(3)]
    d_opacity = (sum(got[c] * color[c] for c in range(3)) + got_share) * far
    d_weight = [
        sum(d_color[c] * radiance[c][s] for c in range(3)) + d_opacity for s in range(SAMPLES)
    ]
    later = jnp.zeros_like(far)
    cot_scr[...] = jnp.zeros_like(cot_scr)
    for s in reversed(range(SAMPLES)):
        d_optical = passed[s] * decay[s] * d_weight[s] - later
        later = later + weight[s] * d_weight[s]
        cot_scr[:, 3, lanes[s]] = d_optical * spacing * gate[s]
        for c in range(3):
            r = radiance[c][s]
            cot_scr[:, c, lanes[s]] = d_color[c] * weight[s] * r * (1.0 - r)


def color_kernel(
    group, tiles, ids_ref, me_ref, rays_ref, center_ref, parts_ref, density_ref, radiance_ref,
    h2_ref, shade_ref, vc_ref, wfdt, wct, wrt, low_ref,
    colors_ref, keep_ref, send_ref, column_ref, d2_ref,
    cot_scr, head_ref, fd_scr, r_scr, vc_scr,
):
    step = pl.program_id(0)

    @pl.when(step == 0)
    def _():
        cotangents(rays_ref, center_ref, parts_ref, density_ref, radiance_ref, cot_scr)
        me = me_ref[0]
        for t in range(tiles):
            summed = [
                sum(parts_ref[ids_ref[t, k], c, pl.ds(me, 1), :] for k in range(3)) for c in range(4)
            ]
            for c in range(3):
                colors_ref[c : c + 1, t * TILE : (t + 1) * TILE] = summed[c] / summed[3]
        for ref in (fd_scr, r_scr, vc_scr):
            ref[...] = jnp.zeros_like(ref)

    for j in range(group):
        tile = step * group + j
        at = slice(j * COLS, (j + 1) * COLS)
        cot = cot_scr[tile]
        low = jnp.concatenate([cot, jnp.zeros_like(cot)], 0).astype(BF16)
        shaded = shade_ref[:, at]
        d_feature = dot(wrt[...], low) * slope(shaded)
        r_scr[...] += dot_nt(low, shaded)
        d_ray = (
            d_feature[:, 0:TILE]
            + d_feature[:, TILE : 2 * TILE]
            + d_feature[:, 2 * TILE : 3 * TILE]
            + d_feature[:, 3 * TILE :]
        ).astype(BF16)
        vc = vc_ref[:, j * TILE : (j + 1) * TILE]
        vc_scr[...] += dot_nt(vc, d_ray)
        lanes = slice(j * TILE, (j + 1) * TILE)
        codes = wct.shape[0]
        column_ref[0:codes, lanes] = dot(wct[...], d_ray).astype(BF16).astype(F32)
        column_ref[codes:, lanes] = jnp.broadcast_to(
            rays_ref[tile, 6:7, :], (column_ref.shape[0] - codes, TILE)
        )
        h2 = h2_ref[:, at]
        edge = jnp.concatenate([d_feature.astype(BF16), low], 0)
        fd_scr[...] += dot_nt(edge, h2)
        d2_ref[:, at] = (dot(wfdt[...], edge) * slope(h2)).astype(BF16)

    @pl.when(step == pl.num_programs(0) - 1)
    def _():
        head_ref[0:EDGE, :] = fd_scr[...]
        head_ref[EDGE - 8 : EDGE, 0:128] = r_scr[0:8, :]
        half = vc_scr.shape[0] // 2
        head_ref[EDGE : EDGE + half, 0:128] = vc_scr[0:half, :]
        head_ref[EDGE : EDGE + half, 128:256] = vc_scr[half:, :]
        h = keep_ref.shape[0]
        halves(low_ref, head_ref[0:h, :], head_ref[h : 2 * h, :], keep_ref, send_ref)


def halves(low_ref, first, second, keep_ref, send_ref):
    low = low_ref[0] == 1
    keep_ref[...] = jnp.where(low, first, second)
    send_ref[...] = jnp.where(low, second, first)


def trunk_kernel(
    group, low_ref, d2_ref, h1_ref, h0_ref, code_ref, w1t, w0t,
    keep1, send1, keep0, send0, grad,
):
    step = pl.program_id(0)
    hid = w1t.shape[0]

    @pl.when(step == 0)
    def _():
        grad[...] = jnp.zeros_like(grad)

    for j in range(group):
        at = slice(j * COLS, (j + 1) * COLS)
        d2, h1 = d2_ref[:, at], h1_ref[:, at]
        grad[0:hid, :] += dot_nt(d2, h1)
        d1 = (dot(w1t[...], d2) * slope(h1)).astype(BF16)
        h0 = h0_ref[:, at]
        grad[hid : 2 * hid, :] += dot_nt(d1, h0)
        d0 = (dot(w0t[...], d1) * slope(h0)).astype(BF16)
        grad[2 * hid :, :] += dot_nt(code_ref[:, at], d0)

    @pl.when(step == pl.num_programs(0) - 1)
    def _():
        h = keep1.shape[0]
        halves(low_ref, grad[0:h, :], grad[h : 2 * h, :], keep1, send1)
        halves(low_ref, grad[2 * h : 3 * h, :], grad[3 * h : 4 * h, :], keep0, send0)


def table_kernel(side_ref, own_ref, near_ref, far0_ref, far1_ref, out_ref, cols, lhs, total):
    side = side_ref[0]
    codes, rays = out_ref.shape[0], own_ref.shape[1]
    other = side + 1 - 2 * (side & 1)
    cols[side] = own_ref[...]
    cols[other] = near_ref[...]
    cols[3 - side] = far0_ref[...]
    cols[3 - other] = far1_ref[...]
    highs = out_ref.shape[1] // LOW
    chunk = lhs.shape[1]
    total[...] = jnp.zeros_like(total)
    for z in range(4):
        for start in range(0, rays, chunk):
            ids = cols[z, codes : codes + 1, start : start + chunk].astype(jnp.int32)
            low, high = ids & (LOW - 1), ids // LOW
            value = cols[z, 0:codes, start : start + chunk].astype(BF16)
            for hi in range(highs):
                lhs[hi * codes : (hi + 1) * codes, :] = jnp.where(high == hi, value, jnp.zeros_like(value))
            hit = (lax.broadcasted_iota(jnp.int32, (LOW, chunk), 0) == low).astype(F32).astype(BF16)
            total[...] += dot_nt(lhs[...], hit)
    for hi in range(highs):
        out_ref[:, hi * LOW : (hi + 1) * LOW] = total[hi * codes : (hi + 1) * codes]


def join(low_ref, mine, other, out_ref):
    low = low_ref[0] == 1
    h = mine.shape[0]
    out_ref[0:h, :] = jnp.where(low, mine[...], other[...])
    out_ref[h : 2 * h, :] = jnp.where(low, other[...], mine[...])


def head_kernel(low_ref, mine, other, density_ref, feature_ref, view_ref, code_ref, rad_ref, head):
    join(low_ref, mine, other, head)
    feature_ref[...] = head[0:128, :]
    density_ref[...] = head[DENSE : DENSE + 1, :]
    for c in range(3):
        rad_ref[c] = head[EDGE - 8 + c : EDGE - 7 + c, 0:128]
    code_ref[...] = head[EDGE : EDGE + VCODE, 0:128]
    for c in range(view_ref.shape[0]):
        view_ref[c] = head[EDGE + c : EDGE + c + 1, 128:256]


def sides_kernel(low_ref, mine1, other1, mine0, other0, trunk_ref, pos_ref, grad):
    h = 2 * mine1.shape[0]
    join(low_ref, mine1, other1, grad.at[0:h])
    join(low_ref, mine0, other0, grad.at[h : 2 * h])
    hid = trunk_ref.shape[1]
    trunk_ref[1] = grad[0:hid, :]
    trunk_ref[0] = grad[hid : 2 * hid, :]
    for c in range(pos_ref.shape[0]):
        pos_ref[c] = grad[2 * hid + c : 2 * hid + c + 1, :]


def shape_of(*dims, dtype=F32):
    return jax.ShapeDtypeStruct(dims, dtype)


def local(
    anchors,
    directions,
    app_ids,
    block_ids,
    color_grad,
    block_centers,
    pos_weight,
    trunk_weight,
    density_weight,
    feature_weight,
    view_weight,
    code_weight,
    radiance_weight,
    code_table,
):
    tiles = block_ids.shape[0]
    blocks = lax.axis_size("blk")
    reps = lax.axis_size("rep")
    assert reps == 4
    group = 2 if blocks % 2 == 0 else 1
    hid = pos_weight.shape[1]
    codes, entries = code_table.shape[1:]
    params = pltpu.CompilerParams(vmem_limit_bytes=58 * 1024 * 1024)

    send = pl.pallas_call(
        functools.partial(send_kernel, tiles),
        out_shape=shape_of(blocks, ROWS, TILE),
        in_specs=[smem()] + [vmem()] * 4,
        out_specs=vmem(),
        scratch_shapes=[pltpu.VMEM((tiles, ROWS, TILE), F32)],
        name="send",
    )(block_ids, anchors, directions, app_ids.reshape(tiles, TILE), color_grad)
    rays = lax.all_to_all(send, "blk", split_axis=0, concat_axis=0, tiled=True)

    trunk = trunk_weight[0]
    positions, views = pos_weight.shape[2], view_weight.shape[2]
    wp, wfd, wvc, wr, stack, w0t, w1t, wfdt, wct, wrt = pl.pallas_call(
        weight_kernel,
        out_shape=tuple(
            shape_of(*dims, dtype=BF16)
            for dims in (
                (hid, 64), (EDGE, hid), (128, 64), (16, 128), (entries // LOW * codes, LOW),
                (hid, hid), (hid, hid), (hid, EDGE), (codes, 128), (128, 16),
            )
        ),
        in_specs=[vmem()] * 8,
        out_specs=(vmem(),) * 10,
        scratch_shapes=[pltpu.VMEM((64, hid), F32), pltpu.VMEM((64, 128), F32)],
        name="weights",
    )(
        pos_weight[0].T, trunk, density_weight, feature_weight[0], view_weight[0].T,
        code_weight[0].T, radiance_weight[0], code_table[0],
    )

    centers = block_centers.T
    n = blocks * COLS
    steps = blocks // group
    wide = lambda rows, cols: pl.BlockSpec((rows, group * cols), lambda i: (0, i))
    saved_shapes = (
        shape_of(64, n, dtype=BF16),
        shape_of(hid, n, dtype=BF16),
        shape_of(hid, n, dtype=BF16),
        shape_of(hid, n, dtype=BF16),
        shape_of(128, n, dtype=BF16),
        shape_of(64, blocks * TILE, dtype=BF16),
        shape_of(2, blocks, COLS),
        shape_of(3, blocks, COLS),
    )
    saved_specs = (
        wide(64, COLS),
        wide(hid, COLS),
        wide(hid, COLS),
        wide(hid, COLS),
        wide(128, COLS),
        wide(64, TILE),
        whole((2, blocks, COLS)),
        whole((3, blocks, COLS)),
    )
    outs = pl.pallas_call(
        functools.partial(forward_kernel, group, codes),
        grid=(steps,),
        out_shape=(shape_of(4, blocks, TILE),) + saved_shapes,
        in_specs=[
            whole(rays.shape),
            smem(),
            whole(wp.shape),
            whole(trunk.shape),
            whole(wfd.shape),
            whole(wvc.shape),
            whole(wr.shape),
            whole(stack.shape),
        ],
        out_specs=(whole((4, blocks, TILE)),) + saved_specs,
        scratch_shapes=[pltpu.VMEM((blocks, COLS), F32), pltpu.VMEM((3, blocks, COLS), F32)],
        compiler_params=params,
        name="forward",
    )(rays, centers, wp, trunk, wfd, wvc, wr, stack)
    partial, saved = outs[0], outs[1:]
    code, h0, h1, h2, shaded, vc, density, radiance = saved
    parts = lax.all_gather(partial, "blk", axis=0, tiled=False)

    me = lax.axis_index("blk").astype(jnp.int32)[None]
    side = lax.axis_index("rep").astype(jnp.int32)[None]
    head_rows, trunk_rows = EDGE + VCODE, 2 * hid + 64
    code_rows = codes + 8
    half = lambda rows, parts: shape_of(rows // (2 * parts), hid)
    low = ((side == 0) | (side == 3)).astype(jnp.int32)
    square = lambda k, m: pl.CostEstimate(flops=2 * k * m * n, bytes_accessed=2 * k * n, transcendentals=k * n)
    colors, keep, send, columns, d2 = pl.pallas_call(
        functools.partial(color_kernel, group, tiles),
        grid=(steps,),
        out_shape=(
            shape_of(3, tiles * TILE),
            half(head_rows, 1),
            half(head_rows, 1),
            shape_of(code_rows, blocks * TILE),
            shape_of(hid, n, dtype=BF16),
        ),
        in_specs=[smem(), smem(), whole(rays.shape), smem(), whole(parts.shape)]
        + [saved_specs[6], saved_specs[7]]
        + list(saved_specs[3:6])
        + [whole(w.shape) for w in (wfdt, wct, wrt)]
        + [smem()],
        out_specs=(
            whole((3, tiles * TILE)),
            whole((head_rows // 2, hid)),
            whole((head_rows // 2, hid)),
            wide(code_rows, TILE),
            wide(hid, COLS),
        ),
        scratch_shapes=[
            pltpu.VMEM((blocks, 8, COLS), F32),
            pltpu.VMEM((head_rows, hid), F32),
            pltpu.VMEM((EDGE, hid), F32),
            pltpu.VMEM((16, 128), F32),
            pltpu.VMEM((64, 128), F32),
        ],
        compiler_params=params,
        cost_estimate=square(hid, 4 * EDGE),
        name="color",
    )(block_ids, me, rays, centers, parts, density, radiance, h2, shaded, vc, wfdt, wct, wrt, low)

    part = half(trunk_rows, 2)
    trunk_call = pl.pallas_call(
        functools.partial(trunk_kernel, group),
        grid=(steps,),
        out_shape=(part,) * 4,
        in_specs=[smem()] + [wide(x, COLS) for x in (hid, hid, hid, 64)] + [whole((hid, hid))] * 2,
        out_specs=(whole(part.shape),) * 4,
        scratch_shapes=[pltpu.VMEM((trunk_rows, hid), F32)],
        compiler_params=params,
        cost_estimate=square(hid, 8 * hid),
        name="trunk",
    )
    keep1, send1, keep0, send0 = trunk_call(low, d2, h1, h0, code, w1t, w0t)

    swap = lambda x: lax.ppermute(x, "rep", [(0, 1), (1, 0), (2, 3), (3, 2)])
    mirror = lambda x: lax.ppermute(x, "rep", [(0, 3), (3, 0), (1, 2), (2, 1)])
    near = swap(columns)
    far0 = mirror(columns)
    far1 = mirror(near)

    def rep_sum(keep, send):
        got = swap(send)
        pair = keep + got
        got = mirror(pair)
        mine = pair + got
        return mine, swap(mine)

    head_sum = rep_sum(keep, send)
    sums = rep_sum(keep1, send1) + rep_sum(keep0, send0)
    rays_n = blocks * TILE
    chunk = min(rays_n, 1024)
    table_call = pl.pallas_call(
        table_kernel,
        out_shape=shape_of(codes, entries),
        in_specs=[smem()] + [vmem()] * 4,
        out_specs=vmem(),
        scratch_shapes=[
            pltpu.VMEM((reps, code_rows, rays_n), F32),
            pltpu.VMEM((entries // LOW * codes, chunk), BF16),
            pltpu.VMEM((entries // LOW * codes, LOW), F32),
        ],
        compiler_params=params,
        name="table",
    )
    table_grad = table_call(side, columns, near, far0, far1)

    heads_call = pl.pallas_call(
        head_kernel,
        out_shape=(
            shape_of(1, hid),
            shape_of(128, hid),
            shape_of(views, 1, 128),
            shape_of(codes, 128),
            shape_of(3, 1, 128),
        ),
        in_specs=[smem()] + [vmem()] * 2,
        out_specs=(vmem(),) * 5,
        scratch_shapes=[pltpu.VMEM((head_rows, hid), F32)],
        name="heads",
    )
    grad_density, grad_feature, grad_view, grad_code, grad_rad = heads_call(low, *head_sum)
    grad_trunk, grad_pos = pl.pallas_call(
        sides_kernel,
        out_shape=(shape_of(2, hid, hid), shape_of(positions, 1, hid)),
        in_specs=[smem()] + [vmem()] * 4,
        out_specs=(vmem(),) * 2,
        scratch_shapes=[pltpu.VMEM((trunk_rows, hid), F32)],
        name="sides",
    )(low, *sums)
    return (
        colors,
        jnp.transpose(grad_pos, (1, 2, 0)),
        grad_trunk[None],
        grad_density,
        grad_feature[None],
        jnp.transpose(grad_view, (1, 2, 0)),
        grad_code.T[None],
        jnp.transpose(grad_rad, (1, 0, 2)),
        table_grad[None],
    )


def solution(mesh):
    return jax.shard_map(
        local,
        mesh=mesh,
        in_specs=(
            P(None, ("blk", "rep")),
            P(None, ("blk", "rep")),
            P(("blk", "rep")),
            P(("blk", "rep"), None),
            P(None, ("blk", "rep")),
            P(None, "blk"),
            P("blk", None, None),
            P("blk", None, None, None),
            P("blk", None),
            P("blk", None, None),
            P("blk", None, None),
            P("blk", None, None),
            P("blk", None, None),
            P("blk", None, None),
        ),
        out_specs=(
            P(None, ("blk", "rep")),
            P("blk", None, None),
            P("blk", None, None, None),
            P("blk", None),
            P("blk", None, None),
            P("blk", None, None),
            P("blk", None, None),
            P("blk", None, None),
            P("blk", None, None),
        ),
        check_vma=False,
    )
```

```python
import functools

import jax
import jax.numpy as jnp
from jax import lax
from jax.experimental import pallas as pl
from jax.experimental.pallas import tpu as pltpu
from jax.sharding import PartitionSpec as P


TILE = 128
SAMPLES = 4
FREQ = 10
VFREQ = 4
COLS = SAMPLES * TILE
LOW = 256
ROWS = 16
VCODE = 32
EDGE = 144
DENSE = 131
GROUP = 8

ray_span = 2.0
loss_scale = 0.03125
spacing = ray_span / SAMPLES

F32 = jnp.float32
BF16 = jnp.bfloat16


def dot(a, b):
    return lax.dot_general(a, b, (((1,), (0,)), ((), ())), preferred_element_type=F32)


def dot_nt(a, b):
    return lax.dot_general(a, b, (((1,), (1,)), ((), ())), preferred_element_type=F32)


def vmem():
    return pl.BlockSpec(memory_space=pltpu.VMEM)


def smem():
    return pl.BlockSpec(memory_space=pltpu.SMEM)


def whole(shape):
    return pl.BlockSpec(shape, lambda i: (0,) * len(shape))


def sin_cos(angle, is_cos):
    turns = jnp.floor(angle * 0.6366197723675814 + 0.5)
    rest = angle - turns * 1.5703125
    rest = rest - turns * 4.837512969970703125e-4
    rest = rest - turns * 7.54978995489188216e-8
    quarter = turns.astype(jnp.int32) + is_cos
    sq = rest * rest
    sine = rest + rest * sq * (
        -1.6666654611e-1 + sq * (8.3321608736e-3 + sq * -1.9515295891e-4)
    )
    cosine = (
        1.0
        - 0.5 * sq
        + sq * sq * (4.166664568298827e-2 + sq * (-1.388731625493765e-3 + sq * 2.443315711809948e-5))
    )
    value = jnp.where((quarter & 1) == 1, cosine, sine)
    return jnp.where((quarter & 2) == 2, -value, value)


def encode(coords, levels, rows):
    n = coords[0].shape[1]
    row = lax.broadcasted_iota(jnp.int32, (rows, n), 0)
    third = (row * 171) >> 9
    coord = row - 3 * third
    base = jnp.where(coord == 0, coords[0], jnp.where(coord == 1, coords[1], coords[2]))
    is_cos = (third > levels).astype(jnp.int32)
    level = jnp.clip(third - 1 - levels * is_cos, 0, levels - 1)
    scale = (1 << level).astype(F32)
    return jnp.where(third == 0, base, sin_cos(base * scale, is_cos))


def softplus(v):
    return jnp.maximum(v, 0.0) + jnp.log(1.0 + jnp.exp(-jnp.abs(v)))


def slope(h):
    return 1.0 - jnp.exp(-h.astype(F32))


def send_kernel(tiles, ids_ref, anchor_ref, dir_ref, app_ref, grad_ref, out_ref, tile_ref):
    row = lax.broadcasted_iota(jnp.int32, out_ref.shape, 1)
    out_ref[...] = jnp.where((row >= 10) & (row < 13), -1.0, 0.0)
    for t in range(tiles):
        lanes = pl.ds(t * TILE, TILE)
        tile_ref[t] = jnp.zeros((ROWS, TILE), F32)
        tile_ref[t, 0:3, :] = anchor_ref[:, lanes]
        tile_ref[t, 3:6, :] = dir_ref[:, lanes]
        tile_ref[t, 6:7, :] = app_ref[t : t + 1, :].astype(F32)
        tile_ref[t, 7:10, :] = grad_ref[:, lanes]
        for k in range(3):
            tile_ref[t, 10 + k : 11 + k, :] = jnp.full((1, TILE), ids_ref[t, k], jnp.int32).astype(F32)
        for k in range(3):
            out_ref[ids_ref[t, k]] = tile_ref[t]


def forward_views(pack, codes, highs):
    top = highs * codes
    side = top + 512 + EDGE
    return (
        pack.at[side : side + 256, 0:64],
        pack.at[top : top + 512, :],
        pack.at[top + 512 : side, :],
        pack.at[side : side + 128, 128:192],
        pack.at[side + 128 : side + 144, 128:256],
        pack.at[0:top, :],
    )


def backward_views(pack, codes):
    return (
        pack.at[0:256, :],
        pack.at[256:512, :],
        pack.at[512:768, 0:EDGE],
        pack.at[768 : 768 + codes, 128:256],
        pack.at[768:896, 0:16],
    )


def weight_kernel(
    center_ref, pos_ref, tw_ref, density_ref, feature_ref, view_ref, cw_ref, rad_ref, table_ref,
    fore_ref, back_ref, spot_ref, pad, narrow,
):
    codes = table_ref.shape[0]
    wp, tw, wfd, wvc, wr, stack = forward_views(fore_ref, codes, table_ref.shape[1] // LOW)
    w0t, w1t, wfdt, wct, wrt = backward_views(back_ref, codes)
    for c in range(3):
        spot_ref[c : c + 1, :] = jnp.full((1, TILE), center_ref[0, c], F32)
    tw[0:256, :] = tw_ref[0]
    tw[256:512, :] = tw_ref[1]
    pad[...] = jnp.zeros_like(pad)
    pad[0 : pos_ref.shape[0], :] = pos_ref[...].astype(F32)
    wp[...] = pad[...].T.astype(BF16)
    narrow[...] = jnp.zeros_like(narrow)
    narrow[0 : cw_ref.shape[0], :] = cw_ref[...].astype(F32)
    narrow[cw_ref.shape[0] : cw_ref.shape[0] + view_ref.shape[0], :] = view_ref[...].astype(F32)
    wvc[...] = narrow[...].T.astype(BF16)
    wct[...] = cw_ref[...]
    wfd[0:128, :] = feature_ref[...]
    pad[0:16, :] = jnp.zeros((16, pad.shape[1]), F32)
    pad[DENSE - 128 : DENSE - 127, :] = density_ref[...].astype(F32)
    wfd[128:EDGE, :] = pad[0 : EDGE - 128, :].astype(BF16)
    narrow[0:16, :] = jnp.zeros((16, narrow.shape[1]), F32)
    narrow[0 : rad_ref.shape[0], :] = rad_ref[...].astype(F32)
    wr[...] = narrow[0:16, :].astype(BF16)
    wrt[...] = wr[...].T
    wfdt[...] = wfd[...].T
    w0t[...] = tw_ref[0].T
    w1t[...] = tw_ref[1].T
    for hi in range(table_ref.shape[1] // LOW):
        stack[hi * codes : (hi + 1) * codes, :] = table_ref[:, hi * LOW : (hi + 1) * LOW]


def composite(density, radiance):
    decay = [jnp.exp(-d * spacing) for d in density]
    passed, run = [], jnp.zeros_like(density[0])
    for d in density:
        passed.append(jnp.exp(-run))
        run = run + d * spacing
    weight = [p * (1.0 - e) for p, e in zip(passed, decay)]
    color = [sum(w * r for w, r in zip(weight, radiance[c])) for c in range(3)]
    return decay, passed, weight, color, sum(weight)


def distance(rays, centers):
    total = 1.0
    for c in range(3):
        offset = rays[:, c, :] - centers[c : c + 1, :]
        total = total + offset * offset
    return total


def forward_kernel(
    group, codes, rays_ref, center_ref, pack_ref,
    partial_ref, code_ref, h0_ref, h1_ref, h2_ref, shade_ref, vc_ref, density_ref, radiance_ref,
    dl_scr, rl_scr,
):
    step = pl.program_id(0)
    highs = (pack_ref.shape[0] - 768 - EDGE) // codes
    wp, tw, wfd, wvc, wr, stack = forward_views(pack_ref, codes, highs)
    tiles = range(group)
    at = [slice(j * COLS, (j + 1) * COLS) for j in tiles]
    rays = [rays_ref[step * group + j] for j in tiles]
    vcs = []
    for j in tiles:
        ids = rays[j][6:7, :].astype(jnp.int32)
        low, high = ids & (LOW - 1), ids // LOW
        hit = (lax.broadcasted_iota(jnp.int32, (LOW, TILE), 0) == low).astype(F32).astype(BF16)
        picked = dot(stack[...], hit)
        app = jnp.zeros((codes, TILE), F32)
        for hi in range(highs):
            app = app + jnp.where(high == hi, picked[hi * codes : (hi + 1) * codes], 0.0)
        view = encode([rays[j][3 + c : 4 + c, :] for c in range(3)], VFREQ, VCODE)
        vcs.append(jnp.concatenate([app, view], 0).astype(BF16))
        vc_ref[:, j * TILE : (j + 1) * TILE] = vcs[j]
    for j in tiles:
        points = []
        for c in range(3):
            base = rays[j][c : c + 1, :]
            move = rays[j][3 + c : 4 + c, :]
            points.append(
                jnp.concatenate(
                    [base + ((s + 0.5) * spacing) * move - center_ref[c : c + 1, :] for s in range(SAMPLES)], 1
                )
            )
        code_ref[:, at[j]] = encode(points, FREQ, code_ref.shape[0]).astype(BF16)
    for j in tiles:
        h0_ref[:, at[j]] = softplus(dot(wp[...], code_ref[:, at[j]])).astype(BF16)
    for j in tiles:
        h1_ref[:, at[j]] = softplus(dot(tw[0:256, :], h0_ref[:, at[j]])).astype(BF16)
    for j in tiles:
        h2_ref[:, at[j]] = softplus(dot(tw[256:512, :], h1_ref[:, at[j]])).astype(BF16)
    for j in tiles:
        per_ray = dot(wvc[...], vcs[j])
        feature = dot(wfd[...], h2_ref[:, at[j]])
        dl_scr[pl.ds(step * group + j, 1), :] = feature[DENSE : DENSE + 1, :]
        shaded = softplus(feature[0:128] + jnp.concatenate([per_ray] * SAMPLES, 1)).astype(BF16)
        shade_ref[:, at[j]] = shaded
    for j in tiles:
        logits = dot(wr[...], shade_ref[:, at[j]])
        for c in range(3):
            rl_scr[c, pl.ds(step * group + j, 1), :] = logits[c : c + 1, :]

    @pl.when(step == pl.num_programs(0) - 1)
    def _():
        logit = dl_scr[...]
        density = jnp.maximum(logit, 0.0) + jnp.log1p(jnp.exp(-jnp.abs(logit)))
        density_ref[0] = density
        density_ref[1] = 1.0 / (1.0 + jnp.exp(-logit))
        radiance = [1.0 / (1.0 + jnp.exp(-rl_scr[c])) for c in range(3)]
        for c in range(3):
            radiance_ref[c] = radiance[c]
        lanes = [slice(s * TILE, (s + 1) * TILE) for s in range(SAMPLES)]
        _, _, _, color, opacity = composite(
            [density[:, at] for at in lanes], [[radiance[c][:, at] for at in lanes] for c in range(3)]
        )
        share = (0.1 + opacity) / distance(rays_ref, center_ref)
        for c in range(3):
            partial_ref[c] = share * color[c]
        partial_ref[3] = share


def cotangents(rays_ref, center_ref, parts_ref, density_ref, radiance_ref, cot_scr):
    ids = [rays_ref[:, 10 + k, :] for k in range(3)]
    live = ids[0] >= 0.0
    summed = [jnp.zeros_like(ids[0]) for _ in range(4)]
    for b in range(parts_ref.shape[0]):
        mine = (ids[0] == b) | (ids[1] == b) | (ids[2] == b)
        for c in range(4):
            summed[c] = summed[c] + jnp.where(mine, parts_ref[b, c], 0.0)
    norm = 1.0 / jnp.where(live, summed[3], 1.0)
    got = [jnp.where(live, rays_ref[:, 7 + c, :] * loss_scale, 0.0) * norm for c in range(3)]
    got_share = -sum(got[c] * summed[c] for c in range(3)) * norm
    lanes = [slice(s * TILE, (s + 1) * TILE) for s in range(SAMPLES)]
    density = [density_ref[0, :, at] for at in lanes]
    gate = [density_ref[1, :, at] for at in lanes]
    radiance = [[radiance_ref[c, :, at] for at in lanes] for c in range(3)]
    decay, passed, weight, color, opacity = composite(density, radiance)
    far = 1.0 / distance(rays_ref, center_ref)
    share = (0.1 + opacity) * far
    d_color = [got[c] * share for c in range(3)]
    d_opacity = (sum(got[c] * color[c] for c in range(3)) + got_share) * far
    d_weight = [
        sum(d_color[c] * radiance[c][s] for c in range(3)) + d_opacity for s in range(SAMPLES)
    ]
    later = jnp.zeros_like(far)
    cot_scr[...] = jnp.zeros_like(cot_scr)
    for s in reversed(range(SAMPLES)):
        d_optical = passed[s] * decay[s] * d_weight[s] - later
        later = later + weight[s] * d_weight[s]
        cot_scr[:, 3, lanes[s]] = d_optical * spacing * gate[s]
        for c in range(3):
            r = radiance[c][s]
            cot_scr[:, c, lanes[s]] = d_color[c] * weight[s] * r * (1.0 - r)


def color_kernel(
    group, tiles, ids_ref, me_ref, rays_ref, center_ref, parts_ref, density_ref, radiance_ref,
    h2_ref, shade_ref, vc_ref, pack_ref, low_ref,
    colors_ref, keep_ref, send_ref, column_ref, d2_ref,
    cot_scr, head_ref, fd_scr, r_scr, vc_scr, edge_scr,
):
    step = pl.program_id(0)

    @pl.when(step == 0)
    def _():
        cotangents(rays_ref, center_ref, parts_ref, density_ref, radiance_ref, cot_scr)
        me = me_ref[0]
        for t in range(tiles):
            summed = [
                sum(parts_ref[ids_ref[t, k], c, pl.ds(me, 1), :] for k in range(3)) for c in range(4)
            ]
            for c in range(3):
                colors_ref[c : c + 1, t * TILE : (t + 1) * TILE] = summed[c] / summed[3]
        for ref in (fd_scr, r_scr, vc_scr):
            ref[...] = jnp.zeros_like(ref)

    codes = column_ref.shape[0] - 8
    _, _, wfdt, wct, wrt = backward_views(pack_ref, codes)
    each = range(group)
    at = [slice(j * COLS, (j + 1) * COLS) for j in each]
    lows, d_rays = [], []
    for j in each:
        cot = cot_scr[step * group + j]
        lows.append(jnp.concatenate([cot, jnp.zeros_like(cot)], 0).astype(BF16))
    for j in each:
        d_feature = dot(wrt[...], lows[j]) * slope(shade_ref[:, at[j]])
        d_rays.append(
            (
                d_feature[:, 0:TILE]
                + d_feature[:, TILE : 2 * TILE]
                + d_feature[:, 2 * TILE : 3 * TILE]
                + d_feature[:, 3 * TILE :]
            ).astype(BF16)
        )
        edge_scr[0:128, at[j]] = d_feature.astype(BF16)
        edge_scr[128:EDGE, at[j]] = lows[j]
    for j in each:
        lanes = slice(j * TILE, (j + 1) * TILE)
        column_ref[0:codes, lanes] = dot(wct[...], d_rays[j]).astype(BF16).astype(F32)
        column_ref[codes:, lanes] = jnp.broadcast_to(
            rays_ref[step * group + j, 6:7, :], (column_ref.shape[0] - codes, TILE)
        )
    for j in each:
        d2_ref[:, at[j]] = (dot(wfdt[...], edge_scr[:, at[j]]) * slope(h2_ref[:, at[j]])).astype(BF16)
    r_scr[...] += dot_nt(edge_scr[128:EDGE, :], shade_ref[...])
    vc_scr[...] += dot_nt(vc_ref[...], jnp.concatenate(d_rays, 1))
    fd_scr[...] += dot_nt(edge_scr[...], h2_ref[...])

    @pl.when(step == pl.num_programs(0) - 1)
    def _():
        head_ref[0:EDGE, :] = fd_scr[...]
        head_ref[EDGE - 8 : EDGE, 0:128] = r_scr[0:8, :]
        half = vc_scr.shape[0] // 2
        head_ref[EDGE : EDGE + half, 0:128] = vc_scr[0:half, :]
        head_ref[EDGE : EDGE + half, 128:256] = vc_scr[half:, :]
        h = keep_ref.shape[0]
        halves(low_ref, head_ref[0:h, :], head_ref[h : 2 * h, :], keep_ref, send_ref)


def halves(low_ref, first, second, keep_ref, send_ref):
    low = low_ref[0] == 1
    keep_ref[...] = jnp.where(low, first, second)
    send_ref[...] = jnp.where(low, second, first)


def trunk_kernel(
    group, low_ref, d2_ref, h1_ref, h0_ref, code_ref, pack_ref,
    keep1, send1, keep0, send0, grad, d1_scr, d0_scr,
):
    step = pl.program_id(0)
    w0t, w1t = backward_views(pack_ref, 32)[0:2]
    hid = d2_ref.shape[0]

    @pl.when(step == 0)
    def _():
        grad[...] = jnp.zeros_like(grad)

    at = [slice(j * COLS, (j + 1) * COLS) for j in range(group)]
    for cols in at:
        d1_scr[:, cols] = (dot(w1t[...], d2_ref[:, cols]) * slope(h1_ref[:, cols])).astype(BF16)
    for cols in at:
        d0_scr[:, cols] = (dot(w0t[...], d1_scr[:, cols]) * slope(h0_ref[:, cols])).astype(BF16)
    grad[0:hid, :] += dot_nt(d2_ref[...], h1_ref[...])
    grad[hid : 2 * hid, :] += dot_nt(d1_scr[...], h0_ref[...])
    grad[2 * hid :, :] += dot_nt(code_ref[...], d0_scr[...])

    @pl.when(step == pl.num_programs(0) - 1)
    def _():
        h = keep1.shape[0]
        halves(low_ref, grad[0:h, :], grad[h : 2 * h, :], keep1, send1)
        halves(low_ref, grad[2 * h : 3 * h, :], grad[3 * h : 4 * h, :], keep0, send0)


def table_kernel(side_ref, own_ref, near_ref, far0_ref, far1_ref, out_ref, cols, lhs, total):
    side = side_ref[0]
    codes, rays = out_ref.shape[0], own_ref.shape[1]
    other = side + 1 - 2 * (side & 1)
    cols[side] = own_ref[...]
    cols[other] = near_ref[...]
    cols[3 - side] = far0_ref[...]
    cols[3 - other] = far1_ref[...]
    highs = out_ref.shape[1] // LOW
    chunk = lhs.shape[1]
    total[...] = jnp.zeros_like(total)
    for z in range(4):
        for start in range(0, rays, chunk):
            ids = cols[z, codes : codes + 1, start : start + chunk].astype(jnp.int32)
            low, high = ids & (LOW - 1), ids // LOW
            value = cols[z, 0:codes, start : start + chunk].astype(BF16)
            for hi in range(highs):
                lhs[hi * codes : (hi + 1) * codes, :] = jnp.where(high == hi, value, jnp.zeros_like(value))
            hit = (lax.broadcasted_iota(jnp.int32, (LOW, chunk), 0) == low).astype(F32).astype(BF16)
            total[...] += dot_nt(lhs[...], hit)
    for hi in range(highs):
        out_ref[:, hi * LOW : (hi + 1) * LOW] = total[hi * codes : (hi + 1) * codes]


def join(low_ref, mine, other, out_ref):
    low = low_ref[0] == 1
    h = mine.shape[0]
    out_ref[0:h, :] = jnp.where(low, mine[...], other[...])
    out_ref[h : 2 * h, :] = jnp.where(low, other[...], mine[...])


def head_kernel(low_ref, mine, other, density_ref, feature_ref, view_ref, code_ref, rad_ref, head):
    join(low_ref, mine, other, head)
    feature_ref[...] = head[0:128, :]
    density_ref[...] = head[DENSE : DENSE + 1, :]
    for c in range(3):
        rad_ref[c] = head[EDGE - 8 + c : EDGE - 7 + c, 0:128]
    code_ref[...] = head[EDGE : EDGE + VCODE, 0:128]
    for c in range(view_ref.shape[0]):
        view_ref[c] = head[EDGE + c : EDGE + c + 1, 128:256]


def sides_kernel(low_ref, mine1, other1, mine0, other0, trunk_ref, pos_ref, grad):
    h = 2 * mine1.shape[0]
    join(low_ref, mine1, other1, grad.at[0:h])
    join(low_ref, mine0, other0, grad.at[h : 2 * h])
    hid = trunk_ref.shape[1]
    trunk_ref[1] = grad[0:hid, :]
    trunk_ref[0] = grad[hid : 2 * hid, :]
    for c in range(pos_ref.shape[0]):
        pos_ref[c] = grad[2 * hid + c : 2 * hid + c + 1, :]


def shape_of(*dims, dtype=F32):
    return jax.ShapeDtypeStruct(dims, dtype)


def local(
    anchors,
    directions,
    app_ids,
    block_ids,
    color_grad,
    block_centers,
    pos_weight,
    trunk_weight,
    density_weight,
    feature_weight,
    view_weight,
    code_weight,
    radiance_weight,
    code_table,
):
    tiles = block_ids.shape[0]
    blocks = lax.axis_size("blk")
    reps = lax.axis_size("rep")
    assert reps == 4
    group = next(g for g in (GROUP, 4, 2, 1) if blocks % g == 0)
    hid = pos_weight.shape[1]
    codes, entries = code_table.shape[1:]
    params = pltpu.CompilerParams(vmem_limit_bytes=30000 * 1024)
    alone = pltpu.CompilerParams(vmem_limit_bytes=60 * 1024 * 1024)
    light = pltpu.CompilerParams(vmem_limit_bytes=8000 * 1024)

    send = pl.pallas_call(
        functools.partial(send_kernel, tiles),
        out_shape=shape_of(blocks, ROWS, TILE),
        in_specs=[smem()] + [vmem()] * 4,
        out_specs=vmem(),
        scratch_shapes=[pltpu.VMEM((tiles, ROWS, TILE), F32)],
        compiler_params=alone,
        name="send",
    )(block_ids, anchors, directions, app_ids.reshape(tiles, TILE), color_grad)
    rays = lax.all_to_all(send, "blk", split_axis=0, concat_axis=0, tiled=True)

    positions, views = pos_weight.shape[2], view_weight.shape[2]
    fore, back, centers = pl.pallas_call(
        weight_kernel,
        out_shape=(
            shape_of(entries // LOW * codes + 768 + EDGE, hid, dtype=BF16),
            shape_of(896, hid, dtype=BF16),
            shape_of(8, TILE),
        ),
        in_specs=[smem()] + [vmem()] * 8,
        out_specs=(vmem(),) * 3,
        scratch_shapes=[pltpu.VMEM((64, hid), F32), pltpu.VMEM((64, 128), F32)],
        compiler_params=alone,
        name="weights",
    )(
        block_centers.T, pos_weight[0].T, trunk_weight[0], density_weight, feature_weight[0],
        view_weight[0].T, code_weight[0].T, radiance_weight[0], code_table[0],
    )

    n = blocks * COLS
    steps = blocks // group
    wide = lambda rows, cols: pl.BlockSpec((rows, group * cols), lambda i: (0, i))
    saved_shapes = (
        shape_of(64, n, dtype=BF16),
        shape_of(hid, n, dtype=BF16),
        shape_of(hid, n, dtype=BF16),
        shape_of(hid, n, dtype=BF16),
        shape_of(128, n, dtype=BF16),
        shape_of(64, blocks * TILE, dtype=BF16),
        shape_of(2, blocks, COLS),
        shape_of(3, blocks, COLS),
    )
    saved_specs = (
        wide(64, COLS),
        wide(hid, COLS),
        wide(hid, COLS),
        wide(hid, COLS),
        wide(128, COLS),
        wide(64, TILE),
        whole((2, blocks, COLS)),
        whole((3, blocks, COLS)),
    )
    outs = pl.pallas_call(
        functools.partial(forward_kernel, group, codes),
        grid=(steps,),
        out_shape=(shape_of(4, blocks, TILE),) + saved_shapes,
        in_specs=[
            whole(rays.shape),
            whole(centers.shape),
            whole(fore.shape),
        ],
        out_specs=(whole((4, blocks, TILE)),) + saved_specs,
        scratch_shapes=[pltpu.VMEM((blocks, COLS), F32), pltpu.VMEM((3, blocks, COLS), F32)],
        compiler_params=params,
        name="forward",
    )(rays, centers, fore)
    partial, saved = outs[0], outs[1:]
    code, h0, h1, h2, shaded, vc, density, radiance = saved
    parts = lax.all_gather(partial, "blk", axis=0, tiled=False)

    me = lax.axis_index("blk").astype(jnp.int32)[None]
    side = lax.axis_index("rep").astype(jnp.int32)[None]
    head_rows, trunk_rows = EDGE + VCODE, 2 * hid + 64
    code_rows = codes + 8
    half = lambda rows, parts: shape_of(rows // (2 * parts), hid)
    low = ((side == 0) | (side == 3)).astype(jnp.int32)
    square = lambda k, m: pl.CostEstimate(flops=2 * k * m * n, bytes_accessed=2 * k * n, transcendentals=k * n)
    colors, keep, send, columns, d2 = pl.pallas_call(
        functools.partial(color_kernel, group, tiles),
        grid=(steps,),
        out_shape=(
            shape_of(3, tiles * TILE),
            half(head_rows, 1),
            half(head_rows, 1),
            shape_of(code_rows, blocks * TILE),
            shape_of(hid, n, dtype=BF16),
        ),
        in_specs=[smem(), smem(), whole(rays.shape), whole(centers.shape), whole(parts.shape)]
        + [saved_specs[6], saved_specs[7]]
        + list(saved_specs[3:6])
        + [whole(back.shape), smem()],
        out_specs=(
            whole((3, tiles * TILE)),
            whole((head_rows // 2, hid)),
            whole((head_rows // 2, hid)),
            wide(code_rows, TILE),
            wide(hid, COLS),
        ),
        scratch_shapes=[
            pltpu.VMEM((blocks, 8, COLS), F32),
            pltpu.VMEM((head_rows, hid), F32),
            pltpu.VMEM((EDGE, hid), F32),
            pltpu.VMEM((16, 128), F32),
            pltpu.VMEM((64, 128), F32),
            pltpu.VMEM((EDGE, group * COLS), BF16),
        ],
        compiler_params=params,
        cost_estimate=square(hid, 4 * EDGE),
        name="color",
    )(block_ids, me, rays, centers, parts, density, radiance, h2, shaded, vc, back, low)

    part = half(trunk_rows, 2)
    trunk_call = pl.pallas_call(
        functools.partial(trunk_kernel, group),
        grid=(steps,),
        out_shape=(part,) * 4,
        in_specs=[smem()] + [wide(x, COLS) for x in (hid, hid, hid, 64)] + [whole(back.shape)],
        out_specs=(whole(part.shape),) * 4,
        scratch_shapes=[pltpu.VMEM((trunk_rows, hid), F32)]
        + [pltpu.VMEM((hid, group * COLS), BF16)] * 2,
        compiler_params=params,
        cost_estimate=square(hid, 8 * hid),
        name="trunk",
    )
    keep1, send1, keep0, send0 = trunk_call(low, d2, h1, h0, code, back)

    swap = lambda x: lax.ppermute(x, "rep", [(0, 1), (1, 0), (2, 3), (3, 2)])
    mirror = lambda x: lax.ppermute(x, "rep", [(0, 3), (3, 0), (1, 2), (2, 1)])
    near = swap(columns)
    far0 = mirror(columns)
    far1 = mirror(near)

    def rep_sum(keep, send):
        got = swap(send)
        pair = keep + got
        got = mirror(pair)
        mine = pair + got
        return mine, swap(mine)

    head_sum = rep_sum(keep, send)
    sums = rep_sum(keep1, send1) + rep_sum(keep0, send0)
    rays_n = blocks * TILE
    chunk = min(rays_n, 1024)
    table_call = pl.pallas_call(
        table_kernel,
        out_shape=shape_of(codes, entries),
        in_specs=[smem()] + [vmem()] * 4,
        out_specs=vmem(),
        scratch_shapes=[
            pltpu.VMEM((reps, code_rows, rays_n), F32),
            pltpu.VMEM((entries // LOW * codes, chunk), BF16),
            pltpu.VMEM((entries // LOW * codes, LOW), F32),
        ],
        compiler_params=params,
        name="table",
    )
    table_grad = table_call(side, columns, near, far0, far1)

    heads_call = pl.pallas_call(
        head_kernel,
        out_shape=(
            shape_of(1, hid),
            shape_of(128, hid),
            shape_of(views, 1, 128),
            shape_of(codes, 128),
            shape_of(3, 1, 128),
        ),
        in_specs=[smem()] + [vmem()] * 2,
        out_specs=(vmem(),) * 5,
        scratch_shapes=[pltpu.VMEM((head_rows, hid), F32)],
        compiler_params=light,
        name="heads",
    )
    grad_density, grad_feature, grad_view, grad_code, grad_rad = heads_call(low, *head_sum)
    grad_trunk, grad_pos = pl.pallas_call(
        sides_kernel,
        out_shape=(shape_of(2, hid, hid), shape_of(positions, 1, hid)),
        in_specs=[smem()] + [vmem()] * 4,
        out_specs=(vmem(),) * 2,
        scratch_shapes=[pltpu.VMEM((trunk_rows, hid), F32)],
        compiler_params=light,
        name="sides",
    )(low, *sums)
    return (
        colors,
        jnp.transpose(grad_pos, (1, 2, 0)),
        grad_trunk[None],
        grad_density,
        grad_feature[None],
        jnp.transpose(grad_view, (1, 2, 0)),
        grad_code.T[None],
        jnp.transpose(grad_rad, (1, 0, 2)),
        table_grad[None],
    )


def solution(mesh):
    return jax.shard_map(
        local,
        mesh=mesh,
        in_specs=(
            P(None, ("blk", "rep")),
            P(None, ("blk", "rep")),
            P(("blk", "rep")),
            P(("blk", "rep"), None),
            P(None, ("blk", "rep")),
            P(None, "blk"),
            P("blk", None, None),
            P("blk", None, None, None),
            P("blk", None),
            P("blk", None, None),
            P("blk", None, None),
            P("blk", None, None),
            P("blk", None, None),
            P("blk", None, None),
        ),
        out_specs=(
            P(None, ("blk", "rep")),
            P("blk", None, None),
            P("blk", None, None, None),
            P("blk", None),
            P("blk", None, None),
            P("blk", None, None),
            P("blk", None, None),
            P("blk", None, None),
            P("blk", None, None),
        ),
        check_vma=False,
    )
```

```python
import functools

import jax
import jax.numpy as jnp
from jax import lax
from jax.experimental import pallas as pl
from jax.experimental.pallas import tpu as pltpu
from jax.sharding import PartitionSpec as P


TILE = 128
SAMPLES = 4
FREQ = 10
VFREQ = 4
COLS = SAMPLES * TILE
LOW = 256
ROWS = 16
VCODE = 32
EDGE = 144
DENSE = 131
GROUP = 8

ray_span = 2.0
loss_scale = 0.03125
spacing = ray_span / SAMPLES

F32 = jnp.float32
BF16 = jnp.bfloat16


def dot(a, b):
    return lax.dot_general(a, b, (((1,), (0,)), ((), ())), preferred_element_type=F32)


def dot_nt(a, b):
    return lax.dot_general(a, b, (((1,), (1,)), ((), ())), preferred_element_type=F32)


def vmem():
    return pl.BlockSpec(memory_space=pltpu.VMEM)


def smem():
    return pl.BlockSpec(memory_space=pltpu.SMEM)


def whole(shape):
    return pl.BlockSpec(shape, lambda i: (0,) * len(shape))


def sin_cos(angle, is_cos):
    turns = jnp.floor(angle * 0.6366197723675814 + 0.5)
    rest = angle - turns * 1.5703125
    rest = rest - turns * 4.837512969970703125e-4
    rest = rest - turns * 7.54978995489188216e-8
    quarter = turns.astype(jnp.int32) + is_cos
    sq = rest * rest
    sine = rest + rest * sq * (
        -1.6666654611e-1 + sq * (8.3321608736e-3 + sq * -1.9515295891e-4)
    )
    cosine = (
        1.0
        - 0.5 * sq
        + sq * sq * (4.166664568298827e-2 + sq * (-1.388731625493765e-3 + sq * 2.443315711809948e-5))
    )
    value = jnp.where((quarter & 1) == 1, cosine, sine)
    return jnp.where((quarter & 2) == 2, -value, value)


def encode(coords, levels, rows):
    n = coords[0].shape[1]
    row = lax.broadcasted_iota(jnp.int32, (rows, n), 0)
    third = (row * 171) >> 9
    coord = row - 3 * third
    base = jnp.where(coord == 0, coords[0], jnp.where(coord == 1, coords[1], coords[2]))
    is_cos = (third > levels).astype(jnp.int32)
    level = jnp.clip(third - 1 - levels * is_cos, 0, levels - 1)
    scale = (1 << level).astype(F32)
    return jnp.where(third == 0, base, sin_cos(base * scale, is_cos))


def softplus(v):
    return jnp.maximum(v, 0.0) + jnp.log(1.0 + jnp.exp(-jnp.abs(v)))


def slope(h):
    return 1.0 - jnp.exp(-h.astype(F32))


def send_kernel(tiles, ids_ref, anchor_ref, dir_ref, app_ref, grad_ref, out_ref, tile_ref):
    row = lax.broadcasted_iota(jnp.int32, out_ref.shape, 1)
    out_ref[...] = jnp.where((row >= 10) & (row < 13), -1.0, 0.0)
    for t in range(tiles):
        lanes = pl.ds(t * TILE, TILE)
        tile_ref[t] = jnp.zeros((ROWS, TILE), F32)
        tile_ref[t, 0:3, :] = anchor_ref[:, lanes]
        tile_ref[t, 3:6, :] = dir_ref[:, lanes]
        tile_ref[t, 6:7, :] = app_ref[t : t + 1, :].astype(F32)
        tile_ref[t, 7:10, :] = grad_ref[:, lanes]
        for k in range(3):
            tile_ref[t, 10 + k : 11 + k, :] = jnp.full((1, TILE), ids_ref[t, k], jnp.int32).astype(F32)
        for k in range(3):
            out_ref[ids_ref[t, k]] = tile_ref[t]


def forward_views(pack, codes, highs):
    top = highs * codes
    side = top + 512 + EDGE
    return (
        pack.at[side : side + 256, 0:64],
        pack.at[top : top + 512, :],
        pack.at[top + 512 : side, :],
        pack.at[side : side + 128, 128:192],
        pack.at[side + 128 : side + 144, 128:256],
        pack.at[0:top, :],
    )


def backward_views(pack, codes):
    at = pack.shape[0] - 896
    return (
        pack.at[at : at + 256, :],
        pack.at[at + 256 : at + 512, :],
        pack.at[at + 512 : at + 768, 0:EDGE],
        pack.at[at + 768 : at + 768 + codes, 128:256],
        pack.at[at + 768 : at + 896, 0:16],
    )


def weight_kernel(
    center_ref, pos_ref, tw_ref, density_ref, feature_ref, view_ref, cw_ref, rad_ref, table_ref,
    pack_ref, spot_ref, pad, narrow,
):
    codes = table_ref.shape[0]
    wp, tw, wfd, wvc, wr, stack = forward_views(pack_ref, codes, table_ref.shape[1] // LOW)
    w0t, w1t, wfdt, wct, wrt = backward_views(pack_ref, codes)
    for c in range(3):
        spot_ref[c : c + 1, :] = jnp.full((1, TILE), center_ref[0, c], F32)
    tw[0:256, :] = tw_ref[0]
    tw[256:512, :] = tw_ref[1]
    pad[...] = jnp.zeros_like(pad)
    pad[0 : pos_ref.shape[0], :] = pos_ref[...].astype(F32)
    wp[...] = pad[...].T.astype(BF16)
    narrow[...] = jnp.zeros_like(narrow)
    narrow[0 : cw_ref.shape[0], :] = cw_ref[...].astype(F32)
    narrow[cw_ref.shape[0] : cw_ref.shape[0] + view_ref.shape[0], :] = view_ref[...].astype(F32)
    wvc[...] = narrow[...].T.astype(BF16)
    wct[...] = cw_ref[...]
    wfd[0:128, :] = feature_ref[...]
    pad[0:16, :] = jnp.zeros((16, pad.shape[1]), F32)
    pad[DENSE - 128 : DENSE - 127, :] = density_ref[...].astype(F32)
    wfd[128:EDGE, :] = pad[0 : EDGE - 128, :].astype(BF16)
    narrow[0:16, :] = jnp.zeros((16, narrow.shape[1]), F32)
    narrow[0 : rad_ref.shape[0], :] = rad_ref[...].astype(F32)
    wr[...] = narrow[0:16, :].astype(BF16)
    wrt[...] = wr[...].T
    wfdt[...] = wfd[...].T
    w0t[...] = tw_ref[0].T
    w1t[...] = tw_ref[1].T
    for hi in range(table_ref.shape[1] // LOW):
        stack[hi * codes : (hi + 1) * codes, :] = table_ref[:, hi * LOW : (hi + 1) * LOW]


def composite(density, radiance):
    decay = [jnp.exp(-d * spacing) for d in density]
    passed, run = [], jnp.zeros_like(density[0])
    for d in density:
        passed.append(jnp.exp(-run))
        run = run + d * spacing
    weight = [p * (1.0 - e) for p, e in zip(passed, decay)]
    color = [sum(w * r for w, r in zip(weight, radiance[c])) for c in range(3)]
    return decay, passed, weight, color, sum(weight)


def distance(rays, centers):
    total = 1.0
    for c in range(3):
        offset = rays[:, c, :] - centers[c : c + 1, :]
        total = total + offset * offset
    return total


def forward_kernel(
    group, codes, rays_ref, center_ref, pack_ref,
    partial_ref, code_ref, h0_ref, h1_ref, h2_ref, shade_ref, vc_ref, density_ref, radiance_ref,
    dl_scr, rl_scr,
):
    step = pl.program_id(0)
    highs = (pack_ref.shape[0] - 896 - 768 - EDGE) // codes
    wp, tw, wfd, wvc, wr, stack = forward_views(pack_ref, codes, highs)
    tiles = range(group)
    at = [slice(j * COLS, (j + 1) * COLS) for j in tiles]
    rays = [rays_ref[step * group + j] for j in tiles]
    vcs = []
    for j in tiles:
        ids = rays[j][6:7, :].astype(jnp.int32)
        low, high = ids & (LOW - 1), ids // LOW
        hit = (lax.broadcasted_iota(jnp.int32, (LOW, TILE), 0) == low).astype(F32).astype(BF16)
        picked = dot(stack[...], hit)
        app = jnp.zeros((codes, TILE), F32)
        for hi in range(highs):
            app = app + jnp.where(high == hi, picked[hi * codes : (hi + 1) * codes], 0.0)
        view = encode([rays[j][3 + c : 4 + c, :] for c in range(3)], VFREQ, VCODE)
        vcs.append(jnp.concatenate([app, view], 0).astype(BF16))
        vc_ref[:, j * TILE : (j + 1) * TILE] = vcs[j]
    for j in tiles:
        points = []
        for c in range(3):
            base = rays[j][c : c + 1, :]
            move = rays[j][3 + c : 4 + c, :]
            points.append(
                jnp.concatenate(
                    [base + ((s + 0.5) * spacing) * move - center_ref[c : c + 1, :] for s in range(SAMPLES)], 1
                )
            )
        code_ref[:, at[j]] = encode(points, FREQ, code_ref.shape[0]).astype(BF16)
    for j in tiles:
        h0_ref[:, at[j]] = softplus(dot(wp[...], code_ref[:, at[j]])).astype(BF16)
    for j in tiles:
        h1_ref[:, at[j]] = softplus(dot(tw[0:256, :], h0_ref[:, at[j]])).astype(BF16)
    for j in tiles:
        h2_ref[:, at[j]] = softplus(dot(tw[256:512, :], h1_ref[:, at[j]])).astype(BF16)
    for j in tiles:
        per_ray = dot(wvc[...], vcs[j])
        feature = dot(wfd[...], h2_ref[:, at[j]])
        dl_scr[pl.ds(step * group + j, 1), :] = feature[DENSE : DENSE + 1, :]
        shaded = softplus(feature[0:128] + jnp.concatenate([per_ray] * SAMPLES, 1)).astype(BF16)
        shade_ref[:, at[j]] = shaded
    for j in tiles:
        logits = dot(wr[...], shade_ref[:, at[j]])
        for c in range(3):
            rl_scr[c, pl.ds(step * group + j, 1), :] = logits[c : c + 1, :]

    @pl.when(step == pl.num_programs(0) - 1)
    def _():
        logit = dl_scr[...]
        density = jnp.maximum(logit, 0.0) + jnp.log1p(jnp.exp(-jnp.abs(logit)))
        density_ref[0] = density
        density_ref[1] = 1.0 / (1.0 + jnp.exp(-logit))
        radiance = [1.0 / (1.0 + jnp.exp(-rl_scr[c])) for c in range(3)]
        for c in range(3):
            radiance_ref[c] = radiance[c]
        lanes = [slice(s * TILE, (s + 1) * TILE) for s in range(SAMPLES)]
        _, _, _, color, opacity = composite(
            [density[:, at] for at in lanes], [[radiance[c][:, at] for at in lanes] for c in range(3)]
        )
        share = (0.1 + opacity) / distance(rays_ref, center_ref)
        for c in range(3):
            partial_ref[c] = share * color[c]
        partial_ref[3] = share


def cotangents(rays_ref, center_ref, parts_ref, density_ref, radiance_ref, cot_scr):
    ids = [rays_ref[:, 10 + k, :] for k in range(3)]
    live = ids[0] >= 0.0
    summed = [jnp.zeros_like(ids[0]) for _ in range(4)]
    for b in range(parts_ref.shape[0]):
        mine = (ids[0] == b) | (ids[1] == b) | (ids[2] == b)
        for c in range(4):
            summed[c] = summed[c] + jnp.where(mine, parts_ref[b, c], 0.0)
    norm = 1.0 / jnp.where(live, summed[3], 1.0)
    got = [jnp.where(live, rays_ref[:, 7 + c, :] * loss_scale, 0.0) * norm for c in range(3)]
    got_share = -sum(got[c] * summed[c] for c in range(3)) * norm
    lanes = [slice(s * TILE, (s + 1) * TILE) for s in range(SAMPLES)]
    density = [density_ref[0, :, at] for at in lanes]
    gate = [density_ref[1, :, at] for at in lanes]
    radiance = [[radiance_ref[c, :, at] for at in lanes] for c in range(3)]
    decay, passed, weight, color, opacity = composite(density, radiance)
    far = 1.0 / distance(rays_ref, center_ref)
    share = (0.1 + opacity) * far
    d_color = [got[c] * share for c in range(3)]
    d_opacity = (sum(got[c] * color[c] for c in range(3)) + got_share) * far
    d_weight = [
        sum(d_color[c] * radiance[c][s] for c in range(3)) + d_opacity for s in range(SAMPLES)
    ]
    later = jnp.zeros_like(far)
    cot_scr[...] = jnp.zeros_like(cot_scr)
    for s in reversed(range(SAMPLES)):
        d_optical = passed[s] * decay[s] * d_weight[s] - later
        later = later + weight[s] * d_weight[s]
        cot_scr[:, 3, lanes[s]] = d_optical * spacing * gate[s]
        for c in range(3):
            r = radiance[c][s]
            cot_scr[:, c, lanes[s]] = d_color[c] * weight[s] * r * (1.0 - r)


def color_kernel(
    group, tiles, ids_ref, me_ref, rays_ref, center_ref, parts_ref, density_ref, radiance_ref,
    h2_ref, shade_ref, vc_ref, pack_ref, low_ref,
    colors_ref, keep_ref, send_ref, column_ref, d2_ref,
    cot_scr, head_ref, fd_scr, r_scr, vc_scr, edge_scr,
):
    step = pl.program_id(0)

    @pl.when(step == 0)
    def _():
        cotangents(rays_ref, center_ref, parts_ref, density_ref, radiance_ref, cot_scr)
        me = me_ref[0]
        for t in range(tiles):
            summed = [
                sum(parts_ref[ids_ref[t, k], c, pl.ds(me, 1), :] for k in range(3)) for c in range(4)
            ]
            for c in range(3):
                colors_ref[c : c + 1, t * TILE : (t + 1) * TILE] = summed[c] / summed[3]
        for ref in (fd_scr, r_scr, vc_scr):
            ref[...] = jnp.zeros_like(ref)

    codes = column_ref.shape[0] - 8
    _, _, wfdt, wct, wrt = backward_views(pack_ref, codes)
    each = range(group)
    at = [slice(j * COLS, (j + 1) * COLS) for j in each]
    lows, d_rays = [], []
    for j in each:
        cot = cot_scr[step * group + j]
        lows.append(jnp.concatenate([cot, jnp.zeros_like(cot)], 0).astype(BF16))
    for j in each:
        d_feature = dot(wrt[...], lows[j]) * slope(shade_ref[:, at[j]])
        d_rays.append(
            (
                d_feature[:, 0:TILE]
                + d_feature[:, TILE : 2 * TILE]
                + d_feature[:, 2 * TILE : 3 * TILE]
                + d_feature[:, 3 * TILE :]
            ).astype(BF16)
        )
        edge_scr[0:128, at[j]] = d_feature.astype(BF16)
        edge_scr[128:EDGE, at[j]] = lows[j]
    for j in each:
        lanes = slice(j * TILE, (j + 1) * TILE)
        column_ref[0:codes, lanes] = dot(wct[...], d_rays[j]).astype(BF16).astype(F32)
        column_ref[codes:, lanes] = jnp.broadcast_to(
            rays_ref[step * group + j, 6:7, :], (column_ref.shape[0] - codes, TILE)
        )
    for j in each:
        d2_ref[:, at[j]] = (dot(wfdt[...], edge_scr[:, at[j]]) * slope(h2_ref[:, at[j]])).astype(BF16)
    r_scr[...] += dot_nt(edge_scr[128:EDGE, :], shade_ref[...])
    vc_scr[...] += dot_nt(vc_ref[...], jnp.concatenate(d_rays, 1))
    fd_scr[...] += dot_nt(edge_scr[...], h2_ref[...])

    @pl.when(step == pl.num_programs(0) - 1)
    def _():
        head_ref[0:EDGE, :] = fd_scr[...]
        head_ref[EDGE - 8 : EDGE, 0:128] = r_scr[0:8, :]
        half = vc_scr.shape[0] // 2
        head_ref[EDGE : EDGE + half, 0:128] = vc_scr[0:half, :]
        head_ref[EDGE : EDGE + half, 128:256] = vc_scr[half:, :]
        h = keep_ref.shape[0]
        halves(low_ref, head_ref[0:h, :], head_ref[h : 2 * h, :], keep_ref, send_ref)


def halves(low_ref, first, second, keep_ref, send_ref):
    low = low_ref[0] == 1
    keep_ref[...] = jnp.where(low, first, second)
    send_ref[...] = jnp.where(low, second, first)


def trunk_kernel(
    group, low_ref, d2_ref, h1_ref, h0_ref, code_ref, pack_ref,
    keep1, send1, keep0, send0, grad, d1_scr, d0_scr,
):
    step = pl.program_id(0)
    w0t, w1t = backward_views(pack_ref, 32)[0:2]
    hid = d2_ref.shape[0]

    @pl.when(step == 0)
    def _():
        grad[...] = jnp.zeros_like(grad)

    at = [slice(j * COLS, (j + 1) * COLS) for j in range(group)]
    for cols in at:
        d1_scr[:, cols] = (dot(w1t[...], d2_ref[:, cols]) * slope(h1_ref[:, cols])).astype(BF16)
    for cols in at:
        d0_scr[:, cols] = (dot(w0t[...], d1_scr[:, cols]) * slope(h0_ref[:, cols])).astype(BF16)
    grad[0:hid, :] += dot_nt(d2_ref[...], h1_ref[...])
    grad[hid : 2 * hid, :] += dot_nt(d1_scr[...], h0_ref[...])
    grad[2 * hid :, :] += dot_nt(code_ref[...], d0_scr[...])

    @pl.when(step == pl.num_programs(0) - 1)
    def _():
        h = keep1.shape[0]
        halves(low_ref, grad[0:h, :], grad[h : 2 * h, :], keep1, send1)
        halves(low_ref, grad[2 * h : 3 * h, :], grad[3 * h : 4 * h, :], keep0, send0)


def table_kernel(side_ref, own_ref, near_ref, far0_ref, far1_ref, out_ref, cols, lhs, total):
    side = side_ref[0]
    codes, rays = out_ref.shape[0], own_ref.shape[1]
    other = side + 1 - 2 * (side & 1)
    cols[side] = own_ref[...]
    cols[other] = near_ref[...]
    cols[3 - side] = far0_ref[...]
    cols[3 - other] = far1_ref[...]
    highs = out_ref.shape[1] // LOW
    chunk = lhs.shape[1]
    total[...] = jnp.zeros_like(total)
    for z in range(4):
        for start in range(0, rays, chunk):
            ids = cols[z, codes : codes + 1, start : start + chunk].astype(jnp.int32)
            low, high = ids & (LOW - 1), ids // LOW
            value = cols[z, 0:codes, start : start + chunk].astype(BF16)
            for hi in range(highs):
                lhs[hi * codes : (hi + 1) * codes, :] = jnp.where(high == hi, value, jnp.zeros_like(value))
            hit = (lax.broadcasted_iota(jnp.int32, (LOW, chunk), 0) == low).astype(F32).astype(BF16)
            total[...] += dot_nt(lhs[...], hit)
    for hi in range(highs):
        out_ref[:, hi * LOW : (hi + 1) * LOW] = total[hi * codes : (hi + 1) * codes]


def join(low_ref, mine, other, out_ref):
    low = low_ref[0] == 1
    h = mine.shape[0]
    out_ref[0:h, :] = jnp.where(low, mine[...], other[...])
    out_ref[h : 2 * h, :] = jnp.where(low, other[...], mine[...])


def head_kernel(low_ref, mine, other, density_ref, feature_ref, view_ref, code_ref, rad_ref, head):
    join(low_ref, mine, other, head)
    feature_ref[...] = head[0:128, :]
    density_ref[...] = head[DENSE : DENSE + 1, :]
    for c in range(3):
        rad_ref[c] = head[EDGE - 8 + c : EDGE - 7 + c, 0:128]
    code_ref[...] = head[EDGE : EDGE + VCODE, 0:128]
    for c in range(view_ref.shape[0]):
        view_ref[c] = head[EDGE + c : EDGE + c + 1, 128:256]


def sides_kernel(low_ref, mine1, other1, mine0, other0, trunk_ref, pos_ref, grad):
    h = 2 * mine1.shape[0]
    join(low_ref, mine1, other1, grad.at[0:h])
    join(low_ref, mine0, other0, grad.at[h : 2 * h])
    hid = trunk_ref.shape[1]
    trunk_ref[1] = grad[0:hid, :]
    trunk_ref[0] = grad[hid : 2 * hid, :]
    for c in range(pos_ref.shape[0]):
        pos_ref[c] = grad[2 * hid + c : 2 * hid + c + 1, :]


def shape_of(*dims, dtype=F32):
    return jax.ShapeDtypeStruct(dims, dtype)


def local(
    anchors,
    directions,
    app_ids,
    block_ids,
    color_grad,
    block_centers,
    pos_weight,
    trunk_weight,
    density_weight,
    feature_weight,
    view_weight,
    code_weight,
    radiance_weight,
    code_table,
):
    tiles = block_ids.shape[0]
    blocks = lax.axis_size("blk")
    reps = lax.axis_size("rep")
    assert reps == 4
    group = next(g for g in (GROUP, 4, 2, 1) if blocks % g == 0)
    hid = pos_weight.shape[1]
    codes, entries = code_table.shape[1:]
    params = pltpu.CompilerParams(vmem_limit_bytes=30000 * 1024)
    alone = pltpu.CompilerParams(vmem_limit_bytes=60 * 1024 * 1024)
    light = pltpu.CompilerParams(vmem_limit_bytes=8000 * 1024)

    send = pl.pallas_call(
        functools.partial(send_kernel, tiles),
        out_shape=shape_of(blocks, ROWS, TILE),
        in_specs=[smem()] + [vmem()] * 4,
        out_specs=vmem(),
        scratch_shapes=[pltpu.VMEM((tiles, ROWS, TILE), F32)],
        compiler_params=alone,
        name="send",
    )(block_ids, anchors, directions, app_ids.reshape(tiles, TILE), color_grad)
    rays = lax.all_to_all(send, "blk", split_axis=0, concat_axis=0, tiled=True)

    positions, views = pos_weight.shape[2], view_weight.shape[2]
    pack, centers = pl.pallas_call(
        weight_kernel,
        out_shape=(
            shape_of(entries // LOW * codes + 768 + EDGE + 896, hid, dtype=BF16),
            shape_of(8, TILE),
        ),
        in_specs=[smem()] + [vmem()] * 8,
        out_specs=(vmem(),) * 2,
        scratch_shapes=[pltpu.VMEM((64, hid), F32), pltpu.VMEM((64, 128), F32)],
        compiler_params=alone,
        name="weights",
    )(
        block_centers.T, pos_weight[0].T, trunk_weight[0], density_weight, feature_weight[0],
        view_weight[0].T, code_weight[0].T, radiance_weight[0], code_table[0],
    )

    n = blocks * COLS
    steps = blocks // group
    wide = lambda rows, cols: pl.BlockSpec((rows, group * cols), lambda i: (0, i))
    saved_shapes = (
        shape_of(64, n, dtype=BF16),
        shape_of(hid, n, dtype=BF16),
        shape_of(hid, n, dtype=BF16),
        shape_of(hid, n, dtype=BF16),
        shape_of(128, n, dtype=BF16),
        shape_of(64, blocks * TILE, dtype=BF16),
        shape_of(2, blocks, COLS),
        shape_of(3, blocks, COLS),
    )
    saved_specs = (
        wide(64, COLS),
        wide(hid, COLS),
        wide(hid, COLS),
        wide(hid, COLS),
        wide(128, COLS),
        wide(64, TILE),
        whole((2, blocks, COLS)),
        whole((3, blocks, COLS)),
    )
    outs = pl.pallas_call(
        functools.partial(forward_kernel, group, codes),
        grid=(steps,),
        out_shape=(shape_of(4, blocks, TILE),) + saved_shapes,
        in_specs=[
            whole(rays.shape),
            whole(centers.shape),
            whole(pack.shape),
        ],
        out_specs=(whole((4, blocks, TILE)),) + saved_specs,
        scratch_shapes=[pltpu.VMEM((blocks, COLS), F32), pltpu.VMEM((3, blocks, COLS), F32)],
        compiler_params=params,
        name="forward",
    )(rays, centers, pack)
    partial, saved = outs[0], outs[1:]
    code, h0, h1, h2, shaded, vc, density, radiance = saved
    parts = lax.all_gather(partial, "blk", axis=0, tiled=False)

    me = lax.axis_index("blk").astype(jnp.int32)[None]
    side = lax.axis_index("rep").astype(jnp.int32)[None]
    head_rows, trunk_rows = EDGE + VCODE, 2 * hid + 64
    code_rows = codes + 8
    half = lambda rows, parts: shape_of(rows // (2 * parts), hid)
    low = ((side == 0) | (side == 3)).astype(jnp.int32)
    square = lambda k, m: pl.CostEstimate(flops=2 * k * m * n, bytes_accessed=2 * k * n, transcendentals=k * n)
    colors, keep, send, columns, d2 = pl.pallas_call(
        functools.partial(color_kernel, group, tiles),
        grid=(steps,),
        out_shape=(
            shape_of(3, tiles * TILE),
            half(head_rows, 1),
            half(head_rows, 1),
            shape_of(code_rows, blocks * TILE),
            shape_of(hid, n, dtype=BF16),
        ),
        in_specs=[smem(), smem(), whole(rays.shape), whole(centers.shape), whole(parts.shape)]
        + [saved_specs[6], saved_specs[7]]
        + list(saved_specs[3:6])
        + [whole(pack.shape), smem()],
        out_specs=(
            whole((3, tiles * TILE)),
            whole((head_rows // 2, hid)),
            whole((head_rows // 2, hid)),
            wide(code_rows, TILE),
            wide(hid, COLS),
        ),
        scratch_shapes=[
            pltpu.VMEM((blocks, 8, COLS), F32),
            pltpu.VMEM((head_rows, hid), F32),
            pltpu.VMEM((EDGE, hid), F32),
            pltpu.VMEM((16, 128), F32),
            pltpu.VMEM((64, 128), F32),
            pltpu.VMEM((EDGE, group * COLS), BF16),
        ],
        compiler_params=params,
        cost_estimate=square(hid, 4 * EDGE),
        name="color",
    )(block_ids, me, rays, centers, parts, density, radiance, h2, shaded, vc, pack, low)

    part = half(trunk_rows, 2)
    trunk_call = pl.pallas_call(
        functools.partial(trunk_kernel, group),
        grid=(steps,),
        out_shape=(part,) * 4,
        in_specs=[smem()] + [wide(x, COLS) for x in (hid, hid, hid, 64)] + [whole(pack.shape)],
        out_specs=(whole(part.shape),) * 4,
        scratch_shapes=[pltpu.VMEM((trunk_rows, hid), F32)]
        + [pltpu.VMEM((hid, group * COLS), BF16)] * 2,
        compiler_params=params,
        cost_estimate=square(hid, 8 * hid),
        name="trunk",
    )
    keep1, send1, keep0, send0 = trunk_call(low, d2, h1, h0, code, pack)

    swap = lambda x: lax.ppermute(x, "rep", [(0, 1), (1, 0), (2, 3), (3, 2)])
    mirror = lambda x: lax.ppermute(x, "rep", [(0, 3), (3, 0), (1, 2), (2, 1)])
    near = swap(columns)
    far0 = mirror(columns)
    far1 = mirror(near)

    def rep_sum(keep, send):
        got = swap(send)
        pair = keep + got
        got = mirror(pair)
        mine = pair + got
        return mine, swap(mine)

    head_sum = rep_sum(keep, send)
    sums = rep_sum(keep1, send1) + rep_sum(keep0, send0)
    rays_n = blocks * TILE
    chunk = min(rays_n, 1024)
    table_call = pl.pallas_call(
        table_kernel,
        out_shape=shape_of(codes, entries),
        in_specs=[smem()] + [vmem()] * 4,
        out_specs=vmem(),
        scratch_shapes=[
            pltpu.VMEM((reps, code_rows, rays_n), F32),
            pltpu.VMEM((entries // LOW * codes, chunk), BF16),
            pltpu.VMEM((entries // LOW * codes, LOW), F32),
        ],
        compiler_params=params,
        name="table",
    )
    table_grad = table_call(side, columns, near, far0, far1)

    heads_call = pl.pallas_call(
        head_kernel,
        out_shape=(
            shape_of(1, hid),
            shape_of(128, hid),
            shape_of(views, 1, 128),
            shape_of(codes, 128),
            shape_of(3, 1, 128),
        ),
        in_specs=[smem()] + [vmem()] * 2,
        out_specs=(vmem(),) * 5,
        scratch_shapes=[pltpu.VMEM((head_rows, hid), F32)],
        compiler_params=light,
        name="heads",
    )
    grad_density, grad_feature, grad_view, grad_code, grad_rad = heads_call(low, *head_sum)
    grad_trunk, grad_pos = pl.pallas_call(
        sides_kernel,
        out_shape=(shape_of(2, hid, hid), shape_of(positions, 1, hid)),
        in_specs=[smem()] + [vmem()] * 4,
        out_specs=(vmem(),) * 2,
        scratch_shapes=[pltpu.VMEM((trunk_rows, hid), F32)],
        compiler_params=light,
        name="sides",
    )(low, *sums)
    return (
        colors,
        jnp.transpose(grad_pos, (1, 2, 0)),
        grad_trunk[None],
        grad_density,
        grad_feature[None],
        jnp.transpose(grad_view, (1, 2, 0)),
        grad_code.T[None],
        jnp.transpose(grad_rad, (1, 0, 2)),
        table_grad[None],
    )


def solution(mesh):
    return jax.shard_map(
        local,
        mesh=mesh,
        in_specs=(
            P(None, ("blk", "rep")),
            P(None, ("blk", "rep")),
            P(("blk", "rep")),
            P(("blk", "rep"), None),
            P(None, ("blk", "rep")),
            P(None, "blk"),
            P("blk", None, None),
            P("blk", None, None, None),
            P("blk", None),
            P("blk", None, None),
            P("blk", None, None),
            P("blk", None, None),
            P("blk", None, None),
            P("blk", None, None),
        ),
        out_specs=(
            P(None, ("blk", "rep")),
            P("blk", None, None),
            P("blk", None, None, None),
            P("blk", None),
            P("blk", None, None),
            P("blk", None, None),
            P("blk", None, None),
            P("blk", None, None),
            P("blk", None, None),
        ),
        check_vma=False,
    )
```
